32 devices in a mesh: io: 16 (over z, x, core), rep: 2 (over y).
Axes of the slice: x: 2, y: 2, z: 4, core: 2. Of those that a mesh axis runs over, the one named last changes fastest.
Arguments:
- snapshots: float32 [49152, 2048], P(('rep', 'io')), parts along dimension 0, may hold values from -6 to 6
Outputs:
- coefficients: float32 [32, 256, 2048], P('rep', None, 'io'), parts along dimension 0
- resid_var: float32 [512, 2048], P('rep', 'io'), parts along dimension 0
The draws below stay inside these ranges and needn't reach their ends.
There are 2 independent parts, one for each index of `rep`. The reference program is written for one: setup_inputs(seed, part) draws one part's arguments, and reference() takes and returns one part's arrays. A program takes and returns all parts, laid end to end along the dimension named above; each array names one. Nothing has to cross between parts.
All inputs are finite; a program needn't handle non-finite values.
Results may differ from the reference program's by a relative error of at most 0.000071.
Values sent between devices are 32-bit elements; how exact they have to be, the bound alone decides.
No kernel may reach another device: no remote copies, remote signals or barrier semaphores. Data moves between devices by JAX's collectives and lax.ppermute only.
A program may use at most 128 MiB of HBM per device.

```python
import jax
import jax.numpy as jnp
from jax import lax

TIMES = 96
HARM = 16
LAT = 256
LON = 2048


def level_of(own_key, dims, cuts, low, top_value):
    def one(axis_at, parts):
        heights = jax.random.uniform(jax.random.fold_in(jax.random.fold_in(own_key, 6), axis_at), (parts,), jnp.float32, low / len(cuts), top_value / len(cuts))
        return jnp.repeat(jnp.exp(heights), dims[axis_at] // parts).reshape((-1,) + (1,) * (len(dims) - axis_at - 1))

    gain = one(*cuts[0])
    for cut in cuts[1:]:
        gain = gain * one(*cut)
    return gain


def normal_values(rng, dims, deviation, bound, cuts=(), dtype=jnp.bfloat16):
    array = deviation * jax.random.normal(rng, dims, jnp.float32)
    if cuts:
        array = array * level_of(rng, dims, cuts, -0.22, 0.18)
    return jnp.clip(array, -bound, bound).astype(dtype)


def setup_inputs(seed: int = 0, part: int = 0) -> dict:
    arg_keys = jax.random.split(jax.random.key(seed), 2)
    part_splits = jax.random.split(jax.random.fold_in(arg_keys[1], part), 2)
    snapshots = normal_values(part_splits[0], (TIMES * LAT, LON), 1.0, 6.0, ((0, 16),), jnp.float32)
    return {"snapshots": snapshots}


def basis_matrix(times):
    steps = jnp.arange(times).astype(jnp.float32)
    columns = [jnp.ones_like(steps), (steps - (times - 1) / 2.0) / (times / 2.0)]
    for harmonic in range(1, 7):
        columns.append(jnp.cos(2.0 * jnp.pi * harmonic * steps / 12.0))
    for harmonic in range(1, 6):
        columns.append(jnp.sin(2.0 * jnp.pi * harmonic * steps / 12.0))
    columns.append(jnp.cos(2.0 * jnp.pi * steps / times))
    columns.append(jnp.sin(2.0 * jnp.pi * steps / times))
    columns.append(jnp.cos(4.0 * jnp.pi * steps / times))
    return jnp.stack(columns, axis=1)

def projector_of(basis):
    gram = jnp.dot(basis.T, basis, precision=lax.Precision.HIGHEST)
    factor = jnp.linalg.cholesky(gram)
    middle = lax.linalg.triangular_solve(factor, basis.T, left_side=True, lower=True)
    return lax.linalg.triangular_solve(factor, middle, left_side=True, lower=True, transpose_a=True)

def reference(snapshots):
    series = snapshots.reshape(TIMES, LAT * LON)
    basis = basis_matrix(TIMES)
    projector = projector_of(basis)
    coeffs = jnp.dot(projector, series, precision=lax.Precision.HIGHEST)
    fitted = jnp.dot(basis, coeffs, precision=lax.Precision.HIGHEST)
    resid = series - fitted
    variance = jnp.mean(resid * resid, axis=0)
    return (coeffs.reshape(HARM, LAT, LON), variance.reshape(LAT, LON))
```

```python
import functools

import jax
import jax.numpy as jnp
import numpy as np
from jax import lax
from jax.experimental import pallas as pl
from jax.experimental.pallas import tpu as pltpu
from jax.sharding import PartitionSpec as P

TIMES = 96
HARM = 16
PERIOD = 12
SLOW = HARM - PERIOD
STATS = HARM + 1
PLANES = 4
CHUNKS = 8


def basis_matrix(times):
    steps = np.arange(times, dtype=np.float64)
    columns = [np.ones_like(steps), (steps - (times - 1) / 2.0) / (times / 2.0)]
    for harmonic in range(1, 7):
        columns.append(np.cos(2.0 * np.pi * harmonic * steps / 12.0))
    for harmonic in range(1, 6):
        columns.append(np.sin(2.0 * np.pi * harmonic * steps / 12.0))
    columns.append(np.cos(2.0 * np.pi * steps / times))
    columns.append(np.sin(2.0 * np.pi * steps / times))
    columns.append(np.cos(4.0 * np.pi * steps / times))
    return np.stack(columns, axis=1)


PERIODIC = [0] + list(range(2, 13))
SLOWS = [1, 13, 14, 15]


def fit_matrices():
    basis = basis_matrix(TIMES)
    to_moments = np.zeros((HARM, HARM))
    for column in PERIODIC:
        to_moments[column, :PERIOD] = basis[:PERIOD, column]
    for at, column in enumerate(SLOWS):
        to_moments[column, PERIOD + at] = 1.0
    to_coeffs = np.linalg.solve(basis.T @ basis, to_moments)
    return to_moments, to_coeffs


def fit_block(block, basis, projector):
    width = block.shape[-1]
    lat_rows = block.shape[0] // TIMES
    series = block.reshape(TIMES, lat_rows * width)
    coeffs = jnp.dot(projector, series, precision=lax.Precision.HIGHEST)
    moments = jnp.dot(basis.T, series, precision=lax.Precision.HIGHEST)
    total = jnp.sum(series * series, axis=0)
    variance = (total - jnp.sum(coeffs * moments, axis=0)) / TIMES
    return coeffs.reshape(HARM, lat_rows, width), variance.reshape(lat_rows, width)


def general(snapshots):
    groups = lax.axis_size("io")
    local_rows = snapshots.shape[0]
    lon_dev = snapshots.shape[1] // groups
    split_view = snapshots.reshape(local_rows, groups, lon_dev)
    basis = basis_matrix(TIMES)
    projector = np.linalg.solve(basis.T @ basis, basis.T)
    moved = lax.all_to_all(split_view, "io", split_axis=1, concat_axis=0, tiled=True)
    return fit_block(moved[:, 0, :], jnp.float32(basis), jnp.float32(projector))


def pack_kernel(held, width, where_ref, x_ref, *outs):
    place = where_ref[0]
    for shift, out in enumerate(outs, start=1):
        column = pl.multiple_of((place ^ shift) * width, width)
        out[0] = x_ref[:, :, pl.ds(column, width)]


def stats_kernel(held, where_ref, weight_ref, own_ref, r1_ref, r2_ref, r3_ref, home_ref, away_ref):
    step = pl.program_id(0)
    place = where_ref[0]
    first = (place % 2) * held
    second = held - first

    def stats(emit):
        sources = (own_ref, r1_ref.at[0], r2_ref.at[0], r3_ref.at[0])
        slow = [None] * SLOW
        square = None
        for k in range(held):
            values = [ref[k] for ref in sources]
            emit(first + k, values[0] + values[2])
            emit(second + k, values[1] + values[3])
            for at, value in enumerate(values):
                for j in range(SLOW):
                    term = value * weight_ref[j, at * held + k]
                    slow[j] = term if slow[j] is None else slow[j] + term
                term = value * value
                square = term if square is None else square + term
        for j in range(SLOW):
            emit(PERIOD + j, slow[j])
        emit(HARM, square)

    @pl.when(step == 0)
    def _():
        def emit(row, value):
            home_ref[row] = value

        stats(emit)

    @pl.when(step > 0)
    def _():
        def emit(row, value):
            away_ref[0, row] = value

        stats(emit)


def merge_kernel(near_a_ref, far_a_ref, near_b_ref, far_b_ref, near_ref, far_ref):
    near_ref[...] = near_a_ref[0] + near_b_ref[0]
    far_ref[...] = far_a_ref[0] + far_b_ref[0]


def final_kernel(to_moments, to_coeffs, where_ref, home_ref, away_ref, a_ref, o_ref, b1_ref, b2_ref, *rest):
    coeff_ref, var_ref = rest[-2:]
    inner = where_ref[1] > 0
    stats = []
    for row in range(STATS):
        kept = jnp.where(inner, away_ref[0, row] + a_ref[0, row], home_ref[row] + o_ref[row])
        stats.append(kept + jnp.where(inner, b1_ref[row], b2_ref[row]))

    def mix(weights):
        total = None
        for weight, stat in zip(weights, stats):
            if weight != 0.0:
                term = stat if weight == 1.0 else stat * np.float32(weight)
                total = term if total is None else total + term
        return total

    explained = None
    for column in range(HARM):
        coeff = mix(to_coeffs[column])
        coeff_ref[column] = coeff
        term = coeff * mix(to_moments[column])
        explained = term if explained is None else explained + term
    var_ref[...] = (stats[HARM] - explained) * np.float32(1.0 / TIMES)


def plane_plan(snapshots):
    groups = lax.axis_size("io")
    plane = groups // PLANES
    held = TIMES // groups
    lat = snapshots.shape[0] // held
    lon = snapshots.shape[1]
    width = lon // groups
    rows = lat // CHUNKS
    view = snapshots.reshape(held, lat, lon)

    me = lax.axis_index("io")
    place, level = me % plane, me // plane
    flip = (level >= PLANES // 2).astype(jnp.int32)
    inner = ((level > 0) & (level < PLANES - 1)).astype(jnp.int32)
    where = jnp.stack([place, inner, flip]).astype(jnp.int32)

    slow = basis_matrix(TIMES)[:, SLOWS].T
    table = np.zeros((groups, SLOW, plane * held), np.float32)
    for device in range(groups):
        for shift in range(plane):
            start = ((device // plane) * plane + ((device % plane) ^ shift)) * held
            table[device, :, shift * held : (shift + 1) * held] = slow[:, start : start + held]
    weights = lax.dynamic_index_in_dim(jnp.asarray(table), me, 0, keepdims=False)

    def zone(step, where_ref):
        return jnp.where(where_ref[2] > 0, PLANES - 1 - step, step)

    def shape(*dims):
        return jax.ShapeDtypeStruct(dims, jnp.float32)

    def cost(flops, moved):
        return pl.CostEstimate(flops=flops, bytes_accessed=moved, transcendentals=0)

    points = rows * width * PLANES

    def pack(chunk):
        return pl.pallas_call(
            functools.partial(pack_kernel, held, width),
            grid_spec=pltpu.PrefetchScalarGridSpec(
                num_scalar_prefetch=1,
                grid=(PLANES,),
                in_specs=[pl.BlockSpec((held, rows, plane * width), lambda s, w: (0, chunk, zone(s, w)))],
                out_specs=[pl.BlockSpec((1, held, rows, width), lambda s, w: (s, 0, 0, 0))] * (plane - 1),
            ),
            out_shape=[shape(PLANES, held, rows, width)] * (plane - 1),
            cost_estimate=cost(points * held, points * held * plane * 8),
            name="pack",
        )(where, view)

    def exchange(packed):
        return [
            lax.ppermute(packed[shift - 1], "io", [(i, i ^ shift) for i in range(groups)])
            for shift in range(1, plane)
        ]

    def statistics(chunk, got):
        part = pl.BlockSpec((1, held, rows, width), lambda s, w: (s, 0, 0, 0))
        return pl.pallas_call(
            functools.partial(stats_kernel, held),
            grid_spec=pltpu.PrefetchScalarGridSpec(
                num_scalar_prefetch=1,
                grid=(PLANES,),
                in_specs=[
                    pl.BlockSpec(memory_space=pltpu.SMEM),
                    pl.BlockSpec((held, rows, width), lambda s, w: (0, chunk, zone(s, w) * plane + w[0])),
                ]
                + [part] * (plane - 1),
                out_specs=[
                    pl.BlockSpec((STATS, rows, width), lambda s, w: (0, 0, 0)),
                    pl.BlockSpec((1, STATS, rows, width), lambda s, w: (jnp.maximum(s - 1, 0), 0, 0, 0)),
                ],
            ),
            out_shape=[shape(STATS, rows, width), shape(PLANES - 1, STATS, rows, width)],
            cost_estimate=cost(points * held * plane * 10, points * (held * plane + STATS) * 4),
            name="stats",
        )(where, weights, view, *got)

    outer_in = [(i, i + plane) for i in range(plane)] + [(i, i - plane) for i in range(groups - plane, groups)]
    inner_out = [(b, a) for a, b in outer_in]
    middle = [(i, i + plane) for i in range(plane, 2 * plane)]
    middle = middle + [(b, a) for a, b in middle]
    across = [(i, i + 2 * plane) for i in range(plane, 2 * plane)]
    across = across + [(i, i - 2 * plane) for i in range(2 * plane, 3 * plane)]

    def merge(away, inward):
        def at(index):
            return pl.BlockSpec((1, STATS, rows, width), lambda s: (index, 0, 0, 0))

        whole = pl.BlockSpec((STATS, rows, width), lambda s: (0, 0, 0))
        return pl.pallas_call(
            merge_kernel,
            grid=(1,),
            in_specs=[at(1), at(2), at(1), at(2)],
            out_specs=[whole, whole],
            out_shape=[shape(STATS, rows, width)] * 2,
            cost_estimate=cost(STATS * rows * width * 2, STATS * rows * width * 24),
            name="merge",
        )(away, away, inward, inward)

    to_moments, to_coeffs = fit_matrices()

    def final(chunk, home, away, inward, outward, near, far, outs):
        whole = pl.BlockSpec((STATS, rows, width), lambda s, w: (0, 0, 0))
        head = pl.BlockSpec((1, STATS, rows, width), lambda s, w: (0, 0, 0, 0))
        kept = [pl.BlockSpec(memory_space=pl.ANY)] * len(outs)
        return pl.pallas_call(
            functools.partial(final_kernel, to_moments, to_coeffs),
            grid_spec=pltpu.PrefetchScalarGridSpec(
                num_scalar_prefetch=1,
                grid=(1,),
                in_specs=[whole, head, head, whole, whole, whole] + kept,
                out_specs=[
                    pl.BlockSpec((HARM, rows, width), lambda s, w: (0, chunk, 0)),
                    pl.BlockSpec((rows, width), lambda s, w: (chunk, 0)),
                ],
            ),
            out_shape=[shape(HARM, lat, width), shape(lat, width)],
            input_output_aliases={7: 0, 8: 1} if outs else {},
            cost_estimate=cost(rows * width * 832, STATS * rows * width * 28),
            name="final",
        )(where, home, away, inward, outward, near, far, *outs)

    got = [exchange(pack(chunk)) for chunk in range(CHUNKS)]
    outs = ()
    for chunk in range(CHUNKS):
        home, away = statistics(chunk, got[chunk])
        inward = lax.ppermute(away, "io", outer_in)
        outward = lax.ppermute(home, "io", inner_out)
        near, far = merge(away, inward)
        near = lax.ppermute(near, "io", middle)
        far = lax.ppermute(far, "io", across)
        outs = final(chunk, home, away, inward, outward, near, far, outs)
    return tuple(outs)


def local(snapshots):
    groups = lax.axis_size("io")
    plane = groups // PLANES
    lat = snapshots.shape[0] * groups // TIMES
    fits = (
        groups % PLANES == 0
        and TIMES % groups == 0
        and plane == 4
        and plane * (TIMES // groups) == 2 * PERIOD
        and lat % (8 * CHUNKS) == 0
        and snapshots.shape[1] % (128 * groups) == 0
    )
    return plane_plan(snapshots) if fits else general(snapshots)


def solution(mesh):
    return jax.shard_map(
        local,
        mesh=mesh,
        in_specs=(P(("rep", "io"), None),),
        out_specs=(P("rep", None, "io"), P("rep", "io")),
        check_vma=False,
    )
```

```python
import functools

import jax
import jax.numpy as jnp
import numpy as np
from jax import lax
from jax.experimental import pallas as pl
from jax.experimental.pallas import tpu as pltpu
from jax.sharding import PartitionSpec as P


TIMES = 96
HARM = 16
PERIOD = 12
SLOW = HARM - PERIOD
STATS = HARM + 1
PLANES = 4

PARTS = (3, 4, 6, 7, 7, 5)
MODES = "ssssdd"
ORDER = " ".join((
    "p0 p1 t0 p2",
    "p3 t1 m0 p4",
    "p5 t2 m1 r0",
    "t3 m2 r1 f0",
    "t4 m3 r2 f1",
    "t5 r3 f2 f3",
    "f4 f5",
)).split()
FINAL_ROWS = 8
VMEM_LIMIT = 8 << 20


def basis_matrix(times):
    steps = np.arange(times, dtype=np.float64)
    columns = [np.ones_like(steps), (steps - (times - 1) / 2.0) / (times / 2.0)]
    for harmonic in range(1, 7):
        columns.append(np.cos(2.0 * np.pi * harmonic * steps / 12.0))
    for harmonic in range(1, 6):
        columns.append(np.sin(2.0 * np.pi * harmonic * steps / 12.0))
    columns.append(np.cos(2.0 * np.pi * steps / times))
    columns.append(np.sin(2.0 * np.pi * steps / times))
    columns.append(np.cos(4.0 * np.pi * steps / times))
    return np.stack(columns, axis=1)


PERIODIC = [0] + list(range(2, 13))
SLOWS = [1, 13, 14, 15]


def fit_matrices():
    basis = basis_matrix(TIMES)
    to_moments = np.zeros((HARM, HARM))
    for column in PERIODIC:
        to_moments[column, :PERIOD] = basis[:PERIOD, column]
    for at, column in enumerate(SLOWS):
        to_moments[column, PERIOD + at] = 1.0
    to_coeffs = np.linalg.solve(basis.T @ basis, to_moments)
    return to_moments, to_coeffs


def fit_block(block, basis, projector):
    width = block.shape[-1]
    lat_rows = block.shape[0] // TIMES
    series = block.reshape(TIMES, lat_rows * width)
    coeffs = jnp.dot(projector, series, precision=lax.Precision.HIGHEST)
    moments = jnp.dot(basis.T, series, precision=lax.Precision.HIGHEST)
    total = jnp.sum(series * series, axis=0)
    variance = (total - jnp.sum(coeffs * moments, axis=0)) / TIMES
    return coeffs.reshape(HARM, lat_rows, width), variance.reshape(lat_rows, width)


def general(snapshots):
    groups = lax.axis_size("io")
    local_rows = snapshots.shape[0]
    lon_dev = snapshots.shape[1] // groups
    split_view = snapshots.reshape(local_rows, groups, lon_dev)
    basis = basis_matrix(TIMES)
    projector = np.linalg.solve(basis.T @ basis, basis.T)
    moved = lax.all_to_all(split_view, "io", split_axis=1, concat_axis=0, tiled=True)
    return fit_block(moved[:, 0, :], jnp.float32(basis), jnp.float32(projector))


def zone_of(mode, step, where_ref):
    if mode == "d":
        return where_ref[3] ^ step
    return jnp.where(where_ref[2] > 0, PLANES - 1 - step, step)


def pack_kernel(first, mode, where_ref, x_ref, *rest):
    plane = 4
    outs, sem = rest[-plane - 2 : -2], rest[-1]
    rows, width = outs[0].shape[2:]
    copies = []
    for shift in (2, 3, 1, 0):
        for step in range(PLANES):
            column = (zone_of(mode, step, where_ref) * plane + (where_ref[0] ^ shift)) * width
            source = x_ref.at[:, pl.ds(first, rows), pl.ds(pl.multiple_of(column, width), width)]
            copies.append(pltpu.make_async_copy(source, outs[shift].at[step], sem))
            copies[-1].start()
    for copy in copies:
        copy.wait()


def totals_kernel(mode, where_ref, weight_ref, own_ref, r1_ref, r2_ref, r3_ref, *rest):
    outs = rest[-(PLANES if mode == "d" else 2) - 1 : -1]
    held, rows = own_ref.shape[1:3]
    size = 16 if rows % 16 == 0 else 8
    first = (where_ref[0] % 2) * held
    second = held - first
    sources = (own_ref, r1_ref, r2_ref, r3_ref)
    for step in range(PLANES):
        out_ref = outs[step] if mode == "d" or step == 0 else outs[1].at[step - 1]

        @pl.loop(0, rows // size)
        def _(block):
            at_rows = pl.ds(pl.multiple_of(block * size, size), size)
            slow = [None] * SLOW
            square = None
            for k in range(held):
                values = [ref[step, k, at_rows] for ref in sources]
                out_ref[first + k, at_rows] = values[0] + values[2]
                out_ref[second + k, at_rows] = values[1] + values[3]
                for at, value in enumerate(values):
                    for j in range(SLOW):
                        term = value * weight_ref[j, at * held + k]
                        slow[j] = term if slow[j] is None else slow[j] + term
                    term = value * value
                    square = term if square is None else square + term
            for j in range(SLOW):
                out_ref[PERIOD + j, at_rows] = slow[j]
            out_ref[HARM, at_rows] = square


def merge_kernel(away_ref, in_ref, *rest):
    rest[-2][...] = away_ref[1:3] + in_ref[1:3]


def relay_kernel(home_ref, b_ref, *rest):
    rest[-2][...] = home_ref[...] + b_ref[1]


def final_kernel(first, mode, to_moments, to_coeffs, where_ref, *refs):
    coeff_out, var_out, _, coeff_ref, var_ref, sem = refs[-6:]
    rows = var_ref.shape[0]

    def solve(load):
        @pl.loop(0, rows // FINAL_ROWS)
        def _(block):
            at_rows = pl.ds(pl.multiple_of(block * FINAL_ROWS, FINAL_ROWS), FINAL_ROWS)
            stats = [load(row, at_rows) for row in range(STATS)]

            def mix(weights):
                total = None
                for weight, stat in zip(weights, stats):
                    if abs(weight) > 1e-12:
                        term = stat if weight == 1.0 else stat * np.float32(weight)
                        total = term if total is None else total + term
                return total

            explained = None
            for column in range(HARM):
                coeff = mix(to_coeffs[column])
                coeff_ref[column, at_rows] = coeff
                term = coeff * mix(to_moments[column])
                explained = term if explained is None else explained + term
            var_ref[at_rows] = (stats[HARM] - explained) * np.float32(1.0 / TIMES)

    if mode == "d":
        parts = refs[:PLANES]
        solve(lambda row, at: (parts[0][row, at] + parts[1][row, at]) + (parts[2][row, at] + parts[3][row, at]))
    else:
        home_ref, away_ref, a_ref, b_ref, c_ref = refs[:5]

        @pl.when(where_ref[1] > 0)
        def _():
            solve(lambda row, at: away_ref[0, row, at] + a_ref[0, row, at] + b_ref[0, row, at])

        @pl.when(where_ref[1] == 0)
        def _():
            solve(lambda row, at: home_ref[row, at] + c_ref[row, at])

    copies = [
        pltpu.make_async_copy(coeff_ref, coeff_out.at[:, pl.ds(first, rows)], sem.at[0]),
        pltpu.make_async_copy(var_ref, var_out.at[pl.ds(first, rows)], sem.at[1]),
    ]
    for copy in copies:
        copy.start()
    for copy in copies:
        copy.wait()


def plane_plan(snapshots):
    groups = lax.axis_size("io")
    plane = groups // PLANES
    held = TIMES // groups
    lat = snapshots.shape[0] // held
    lon = snapshots.shape[1]
    width = lon // groups
    view = snapshots.reshape(held, lat, lon)

    me = lax.axis_index("io")
    place, level = me % plane, me // plane
    flip = (level >= PLANES // 2).astype(jnp.int32)
    inner = ((level > 0) & (level < PLANES - 1)).astype(jnp.int32)
    where = jnp.stack([place, inner, flip, level]).astype(jnp.int32)

    slow = basis_matrix(TIMES)[:, SLOWS].T
    table = np.zeros((groups, SLOW, plane * held), np.float32)
    for device in range(groups):
        for shift in range(plane):
            start = ((device // plane) * plane + ((device % plane) ^ shift)) * held
            table[device, :, shift * held : (shift + 1) * held] = slow[:, start : start + held]
    weights = lax.dynamic_index_in_dim(jnp.asarray(table), me, 0, keepdims=False)

    smem = pl.BlockSpec(memory_space=pltpu.SMEM)
    vmem = pl.BlockSpec(memory_space=pltpu.VMEM)
    hbm = pl.BlockSpec(memory_space=pltpu.HBM)
    space = {id(vmem): pltpu.VMEM, id(hbm): pltpu.HBM}
    token = []

    def near(*dims):
        return pltpu.VMEM(dims, jnp.float32)

    def call(kernel, flops, moved, ins, args, outs, out_specs, **more):
        ins, args = ins + [hbm] * len(token), list(args) + token
        args = [
            pltpu.with_memory_space_constraint(arg, space[id(spec)]) if id(spec) in space else arg
            for spec, arg in zip(ins, args)
        ]
        *results, last = pl.pallas_call(
            kernel,
            in_specs=ins,
            out_specs=out_specs + [hbm],
            out_shape=outs + [pltpu.HBM((8, 128), jnp.float32)],
            cost_estimate=pl.CostEstimate(flops=flops, bytes_accessed=moved, transcendentals=0),
            compiler_params=pltpu.CompilerParams(vmem_limit_bytes=VMEM_LIMIT),
            **more,
        )(*args)
        token[:] = [last]
        return results

    def move(value, pairs):
        return lax.ppermute(value, "io", pairs)

    sizes = [part * lat // sum(PARTS) for part in PARTS]
    firsts = [sum(sizes[:chunk]) for chunk in range(len(sizes))]
    swaps = [[(i, i ^ shift) for i in range(groups)] for shift in range(plane)]
    hops = [[(i, i ^ (step * plane)) for i in range(groups)] for step in range(PLANES)]
    to_inner = [(i, i + plane) for i in range(plane)] + [(i, i - plane) for i in range(groups - plane, groups)]
    to_outer = [(b, a) for a, b in to_inner]
    middle = [(i, i + plane) for i in range(plane, 2 * plane)]
    middle = middle + [(b, a) for a, b in middle]
    to_moments, to_coeffs = fit_matrices()

    packed, kept, got, outs = {}, {}, {}, []
    for item in ORDER:
        kind, chunk = item[0], int(item[1:])
        first, rows, mode = firsts[chunk], sizes[chunk], MODES[chunk]
        piece = rows * width
        if kind == "p":
            parts = call(
                functools.partial(pack_kernel, first, mode), piece * held, piece * PLANES * held * plane * 8,
                [smem, hbm], [where, view], [near(PLANES, held, rows, width)] * plane, [vmem] * plane,
                scratch_shapes=[pltpu.SemaphoreType.DMA],
            )
            packed[chunk] = [None] * plane
            packed[chunk][0] = parts[0]
            for shift in (2, 3, 1):
                packed[chunk][shift] = move(parts[shift], swaps[shift])
        elif kind == "t":
            one = near(STATS, rows, width)
            kept[chunk] = call(
                functools.partial(totals_kernel, mode), piece * PLANES * held * plane * 10, piece * 164 * 4,
                [smem, smem] + [vmem] * plane, [where, weights, *packed[chunk]],
                [one] * PLANES if mode == "d" else [one, near(PLANES - 1, STATS, rows, width)],
                [vmem] * (PLANES if mode == "d" else 2),
            )
            if mode == "d":
                for step in (3, 2, 1):
                    kept[chunk][step] = move(kept[chunk][step], hops[step])
            else:
                got[chunk] = [move(kept[chunk][1], to_inner)]
        elif kind == "m":
            (both,) = call(
                merge_kernel, piece * 34, piece * 34 * 12,
                [vmem, vmem], [kept[chunk][1], got[chunk][0]], [near(2, STATS, rows, width)], [vmem],
            )
            got[chunk].append(move(both, middle))
        elif kind == "r":
            (one,) = call(
                relay_kernel, piece * 17, piece * 17 * 12,
                [vmem, vmem], [kept[chunk][0], got[chunk][1]], [near(STATS, rows, width)], [vmem],
            )
            got[chunk].append(move(one, to_outer))
        else:
            args = [*kept[chunk], *got.get(chunk, [])]
            outs = call(
                functools.partial(final_kernel, first, mode, to_moments, to_coeffs), piece * 832, piece * 272,
                [smem] + [vmem] * len(args) + [hbm] * len(outs), [where, *args, *outs],
                [pltpu.HBM((HARM, lat, width), jnp.float32), pltpu.HBM((lat, width), jnp.float32)], [hbm, hbm],
                input_output_aliases={len(args) + 1: 0, len(args) + 2: 1} if outs else {},
                scratch_shapes=[
                    pltpu.VMEM((HARM, rows, width), jnp.float32),
                    pltpu.VMEM((rows, width), jnp.float32),
                    pltpu.SemaphoreType.DMA((2,)),
                ],
            )
    return tuple(outs)


def fits(groups):
    return groups == 4 * PLANES and TIMES % groups == 0 and TIMES // PLANES == 2 * PERIOD


def local(snapshots):
    groups = lax.axis_size("io")
    lat = snapshots.shape[0] * groups // TIMES
    if fits(groups) and lat % (8 * sum(PARTS)) == 0 and snapshots.shape[1] == 128 * groups:
        return plane_plan(snapshots)
    return general(snapshots)


def solution(mesh):
    return jax.shard_map(
        local,
        mesh=mesh,
        in_specs=(P(("rep", "io"), None),),
        out_specs=(P("rep", None, "io"), P("rep", "io")),
        check_vma=False,
    )
```

```python
import functools

import jax
import jax.numpy as jnp
import numpy as np
from jax import lax
from jax.experimental import pallas as pl
from jax.experimental.pallas import tpu as pltpu
from jax.sharding import PartitionSpec as P


TIMES = 96
HARM = 16
PERIOD = 12
SLOW = HARM - PERIOD
STATS = HARM + 1
PLANES = 4

ROUND = 3
PARTS = (7, 5, 7, 6, 4)
GROUPS = (("s", (0,)), ("s", (1,)), ("s", (2,)), ("s", (3,)), ("e", (4,)))
NEARS = ((0, 1), (2, 3, 4))
PAIRS = ((0,), (1, 2, 3, 4))
ORDER = " ".join((
    "p0 P0 q0 p1",
    "q1 p2 p3 p4",
    "t0 T0 t1 n0",
    "m0 m1 t2 r0",
    "r1 f0 t3 m2",
    "f1 t4 n1 m3",
    "F0 r2 m4 r3",
    "f2 f3 f4",
)).split()
FINAL_ROWS = 8
VMEM_LIMIT = 8 << 20


def basis_matrix(times):
    steps = np.arange(times, dtype=np.float64)
    columns = [np.ones_like(steps), (steps - (times - 1) / 2.0) / (times / 2.0)]
    for harmonic in range(1, 7):
        columns.append(np.cos(2.0 * np.pi * harmonic * steps / 12.0))
    for harmonic in range(1, 6):
        columns.append(np.sin(2.0 * np.pi * harmonic * steps / 12.0))
    columns.append(np.cos(2.0 * np.pi * steps / times))
    columns.append(np.sin(2.0 * np.pi * steps / times))
    columns.append(np.cos(4.0 * np.pi * steps / times))
    return np.stack(columns, axis=1)


PERIODIC = [0] + list(range(2, 13))
SLOWS = [1, 13, 14, 15]


def fit_matrices():
    basis = basis_matrix(TIMES)
    to_moments = np.zeros((HARM, HARM))
    for column in PERIODIC:
        to_moments[column, :PERIOD] = basis[:PERIOD, column]
    for at, column in enumerate(SLOWS):
        to_moments[column, PERIOD + at] = 1.0
    to_coeffs = np.linalg.solve(basis.T @ basis, to_moments)
    return to_moments, to_coeffs


def fit_block(block, basis, projector):
    width = block.shape[-1]
    lat_rows = block.shape[0] // TIMES
    series = block.reshape(TIMES, lat_rows * width)
    coeffs = jnp.dot(projector, series, precision=lax.Precision.HIGHEST)
    moments = jnp.dot(basis.T, series, precision=lax.Precision.HIGHEST)
    total = jnp.sum(series * series, axis=0)
    variance = (total - jnp.sum(coeffs * moments, axis=0)) / TIMES
    return coeffs.reshape(HARM, lat_rows, width), variance.reshape(lat_rows, width)


def general(snapshots):
    groups = lax.axis_size("io")
    local_rows = snapshots.shape[0]
    lon_dev = snapshots.shape[1] // groups
    split_view = snapshots.reshape(local_rows, groups, lon_dev)
    basis = basis_matrix(TIMES)
    projector = np.linalg.solve(basis.T @ basis, basis.T)
    moved = lax.all_to_all(split_view, "io", split_axis=1, concat_axis=0, tiled=True)
    return fit_block(moved[:, 0, :], jnp.float32(basis), jnp.float32(projector))


def fetch_kernel(pieces, where_ref, x_ref, *rest):
    outs, sem = rest[-1 - pieces(None) - 1 : -2], rest[-1]
    copies = []
    for out, to_rows, first, rows, at, column in pieces(where_ref):
        ref = outs[out] if at is None else outs[out].at[at]
        width = ref.shape[-1]
        source = x_ref.at[:, pl.ds(first, rows), pl.ds(pl.multiple_of(column, width), width)]
        copies.append(pltpu.make_async_copy(source, ref.at[:, pl.ds(to_rows, rows)], sem))
        copies[-1].start()
    for copy in copies:
        copy.wait()


def sums(values, weights, way, emit):
    slow, square = [None] * SLOW, None
    held = len(values[0])
    for k in range(held):
        for at, source in enumerate(values):
            for j in range(SLOW):
                term = source[k] * weights[way * SLOW + j, at * held + k]
                slow[j] = term if slow[j] is None else slow[j] + term
            term = source[k] * source[k]
            square = term if square is None else square + term
    for j in range(SLOW):
        emit(j, slow[j])
    emit(SLOW, square)


def row_blocks(rows, body):
    size = 16 if rows % 16 == 0 else 8

    @pl.loop(0, rows // size)
    def _(block):
        body(block * size, size)


def totals_kernel(offset, where_ref, weight_ref, own_ref, r1_ref, r2_ref, r3_ref, *rest):
    home_ref, near_ref, far_ref = rest[-4:-1]
    held, rows = own_ref.shape[1:3]
    first = (where_ref[0] % 2) * held
    second = held - first
    for step in range(PLANES):
        out_ref = (home_ref, near_ref, far_ref.at[0], far_ref.at[1])[step]

        def body(start, size):
            at, at1 = pl.ds(pl.multiple_of(start, 8), size), pl.ds(pl.multiple_of(start + offset, 8), size)
            values = [
                [ref[step, k, rows_] for k in range(held)]
                for ref, rows_ in ((own_ref, at), (r1_ref, at1), (r2_ref, at), (r3_ref, at))
            ]
            for k in range(held):
                out_ref[first + k, at] = values[0][k] + values[2][k]
                out_ref[second + k, at] = values[1][k] + values[3][k]

            def emit(row, value):
                out_ref[PERIOD + row, at] = value

            sums(values, weight_ref, 0, emit)

        row_blocks(rows, body)


def round_kernel(where_ref, weight_ref, *rest):
    sources, outs = rest[:PLANES], rest[-5:-1]
    held, rows = sources[0].shape[:2]
    width = outs[0].shape[-1]
    for shift, out_ref in enumerate(outs):
        column = pl.ds(pl.multiple_of((where_ref[0] ^ shift) * width, width), width)

        def body(start, size):
            at = pl.ds(pl.multiple_of(start, 8), size)
            values = [[ref[k, at, column] for k in range(held)] for ref in sources]
            for k in range(held):
                out_ref[k, at] = (values[0][k] + values[1][k]) + (values[2][k] + values[3][k])

            def emit(row, value):
                out_ref[held + row, at] = value

            sums(values, weight_ref, 1, emit)

        row_blocks(rows, body)


def join_kernel(count, *refs):
    out_ref, start = refs[-2], 0
    for ref in refs[:count]:
        rows = ref.shape[1]
        out_ref[:, start : start + rows] = ref[...]
        start += rows


def merge_kernel(count, straight, *refs):
    outs, start = refs[-3:-1] if straight else refs[-2:-1], 0
    for own_ref, in_ref in zip(refs[:count], refs[count : 2 * count]):
        rows = own_ref.shape[2]
        for hop in range(2):
            out_ref = outs[hop] if straight else outs[0].at[hop]
            out_ref[:, start : start + rows] = own_ref[hop] + in_ref[hop]
        start += rows


def relay_kernel(count, b_ref, *refs):
    out_ref, start = refs[-2], 0
    for ref in refs[:count]:
        rows = ref.shape[1]
        out_ref[:, start : start + rows] = ref[...] + b_ref[1, :, start : start + rows]
        start += rows


def solve(matrices, coeff_ref, var_ref, start, rows, load):
    to_moments, to_coeffs = matrices

    @pl.loop(0, rows // FINAL_ROWS)
    def _(block):
        at = pl.multiple_of(block * FINAL_ROWS, FINAL_ROWS)
        stats = [load(row, at) for row in range(STATS)]

        def mix(weights):
            total = None
            for weight, stat in zip(weights, stats):
                if abs(weight) > 1e-12:
                    term = stat if weight == 1.0 else stat * np.float32(weight)
                    total = term if total is None else total + term
            return total

        to = pl.ds(pl.multiple_of(start + at, FINAL_ROWS), FINAL_ROWS)
        explained = None
        for column in range(HARM):
            coeff = mix(to_coeffs[column])
            coeff_ref[column, to] = coeff
            term = coeff * mix(to_moments[column])
            explained = term if explained is None else explained + term
        var_ref[to] = (stats[HARM] - explained) * np.float32(1.0 / TIMES)


def store(first, coeff_out, var_out, coeff_ref, var_ref, sem):
    rows = var_ref.shape[0]
    copies = [
        pltpu.make_async_copy(coeff_ref, coeff_out.at[:, pl.ds(first, rows)], sem.at[0]),
        pltpu.make_async_copy(var_ref, var_out.at[pl.ds(first, rows)], sem.at[1]),
    ]
    for copy in copies:
        copy.start()
    for copy in copies:
        copy.wait()


def final_kernel(first, chunks, mode, matrices, where_ref, *refs):
    coeff_out, var_out, _, coeff_ref, var_ref, sem = refs[-6:]
    count = len(chunks)
    homes, owns, nears = refs[:count], refs[count : 2 * count], refs[2 * count : 3 * count]
    one_ref, two_ref = refs[3 * count : 3 * count + 2]

    @pl.when(where_ref[1] > 0)
    def _():
        start = 0
        for (rows, place), own_ref, in_ref in zip(chunks, owns, nears):

            def load(row, at, start=start, place=place, own_ref=own_ref, in_ref=in_ref):
                middle = one_ref if mode == "e" else one_ref.at[0]
                value = own_ref[row, pl.ds(at, FINAL_ROWS)] + in_ref[row, pl.ds(pl.multiple_of(at + place, 8), FINAL_ROWS)]
                return value + middle[row, pl.ds(pl.multiple_of(at + start, 8), FINAL_ROWS)]

            solve(matrices, coeff_ref, var_ref, start, rows, load)
            start += rows

    @pl.when(where_ref[1] == 0)
    def _():
        start = 0
        for (rows, place), home_ref in zip(chunks, homes):

            def load(row, at, start=start, home_ref=home_ref):
                value = home_ref[row, pl.ds(at, FINAL_ROWS)] + two_ref[row, pl.ds(pl.multiple_of(at + start, 8), FINAL_ROWS)]
                if mode == "e":
                    value = value + refs[3 * count + 2][row, pl.ds(at, FINAL_ROWS)]
                return value

            solve(matrices, coeff_ref, var_ref, start, rows, load)
            start += rows

    store(first, coeff_out, var_out, coeff_ref, var_ref, sem)


def round_final_kernel(held, matrices, where_ref, *refs):
    coeff_out, var_out, _, coeff_ref, var_ref, sem = refs[-6:]
    rows = var_ref.shape[0]

    def run(early, late):
        def load(row, at):
            rows_ = pl.ds(at, FINAL_ROWS)
            if row < PERIOD:
                one, two = early if row < held else late
                return one[row % held, rows_] + two[row % held, rows_]
            row = row - PERIOD + held
            return (refs[0][row, rows_] + refs[1][row, rows_]) + (refs[2][row, rows_] + refs[3][row, rows_])

        solve(matrices, coeff_ref, var_ref, 0, rows, load)

    @pl.when(where_ref[0] % 2 == 0)
    def _():
        run((refs[0], refs[2]), (refs[1], refs[3]))

    @pl.when(where_ref[0] % 2 == 1)
    def _():
        run((refs[1], refs[3]), (refs[0], refs[2]))

    store(0, coeff_out, var_out, coeff_ref, var_ref, sem)


def plane_plan(snapshots):
    groups = lax.axis_size("io")
    plane = groups // PLANES
    held = TIMES // groups
    lat = snapshots.shape[0] // held
    lon = snapshots.shape[1]
    width = lon // groups
    view = snapshots.reshape(held, lat, lon)

    me = lax.axis_index("io")
    place, level = me % plane, me // plane
    flip = (level >= PLANES // 2).astype(jnp.int32)
    inner = ((level > 0) & (level < PLANES - 1)).astype(jnp.int32)
    where = jnp.stack([place, inner, flip, level]).astype(jnp.int32)

    slow = basis_matrix(TIMES)[:, SLOWS].T
    table = np.zeros((groups, 2 * SLOW, plane * held), np.float32)
    for device in range(groups):
        for shift in range(plane):
            for way, other in enumerate((device ^ shift, device ^ (shift * plane))):
                rows, columns = way * SLOW, shift * held
                table[device, rows : rows + SLOW, columns : columns + held] = slow[:, other * held : (other + 1) * held]
    weights = lax.dynamic_index_in_dim(jnp.asarray(table), me, 0, keepdims=False)
    matrices = fit_matrices()

    smem = pl.BlockSpec(memory_space=pltpu.SMEM)
    vmem = pl.BlockSpec(memory_space=pltpu.VMEM)
    hbm = pl.BlockSpec(memory_space=pltpu.HBM)
    space = {id(vmem): pltpu.VMEM, id(hbm): pltpu.HBM}
    token = [weights]

    def near(*dims):
        return pltpu.VMEM(dims, jnp.float32)

    def call(kernel, flops, moved, ins, args, outs, out_specs=None, **more):
        ins, args = ins + [hbm] * len(token), list(args) + token
        args = [
            pltpu.with_memory_space_constraint(arg, space[id(spec)]) if id(spec) in space else arg
            for spec, arg in zip(ins, args)
        ]
        *results, last = pl.pallas_call(
            kernel,
            in_specs=ins,
            out_specs=(out_specs or [vmem] * len(outs)) + [hbm],
            out_shape=outs + [pltpu.HBM((8, 128), jnp.float32)],
            cost_estimate=pl.CostEstimate(flops=flops, bytes_accessed=moved, transcendentals=0),
            compiler_params=pltpu.CompilerParams(vmem_limit_bytes=VMEM_LIMIT),
            **more,
        )(*args)
        token[:] = [last]
        return results

    def move(value, pairs):
        return lax.ppermute(value, "io", pairs)

    unit = lat // (ROUND + sum(PARTS))
    sizes = [part * unit for part in PARTS]
    firsts = [(ROUND + sum(PARTS[:chunk])) * unit for chunk in range(len(PARTS))]
    turn = ROUND * unit
    swaps = [[(i, i ^ shift) for i in range(groups)] for shift in range(plane)]
    hops = [[(i, i ^ (step * plane)) for i in range(groups)] for step in range(PLANES)]
    to_inner = [(i, i + plane) for i in range(plane)] + [(i, i - plane) for i in range(groups - plane, groups)]
    to_outer = [(b, a) for a, b in to_inner]
    middle = [(i, i + plane) for i in range(plane, 2 * plane)]
    middle = middle + [(b, a) for a, b in middle]
    across = [(i, i + 2 * plane) for i in range(plane, 2 * plane)]
    across = across + [(i, i - 2 * plane) for i in range(2 * plane, 3 * plane)]

    def fetch(outs, pieces, rows):
        def count_or_pieces(where_ref):
            return len(outs) if where_ref is None else pieces(where_ref)

        return call(
            functools.partial(fetch_kernel, count_or_pieces), rows * lon, rows * lon * held * 8,
            [smem, hbm], [where, view], outs, scratch_shapes=[pltpu.SemaphoreType.DMA],
        )

    def column(where_ref, step, shift):
        zone = jnp.where(where_ref[2] > 0, PLANES - 1 - step, step)
        return (zone * plane + (where_ref[0] ^ shift)) * width

    def finish(kernel, rows, args, outs):
        count = len(args)
        return call(
            kernel, rows * width * 832, rows * width * 272,
            [smem] + [vmem] * count + [hbm] * len(outs), [where, *args, *outs],
            [pltpu.HBM((HARM, lat, width), jnp.float32), pltpu.HBM((lat, width), jnp.float32)], [hbm, hbm],
            input_output_aliases={count + 1: 0, count + 2: 1} if outs else {},
            scratch_shapes=[
                pltpu.VMEM((HARM, rows, width), jnp.float32),
                pltpu.VMEM((rows, width), jnp.float32),
                pltpu.SemaphoreType.DMA((2,)),
            ],
        )

    packed, paired, home, own, far, moved, outs = {}, {}, {}, {}, {}, {}, []
    for item in ORDER:
        kind, at = item[0], int(item[1:])
        if kind == "P":
            parts = fetch(
                [near(held, turn, plane * width)] * PLANES,
                lambda w: [(step, 0, 0, turn, None, (w[3] ^ step) * plane * width) for step in (3, 2, 1, 0)], turn,
            )
            around = [move(parts[step], hops[step]) for step in (3, 2, 1)]
            around = parts[:1] + around[::-1]
        elif kind == "T":
            parts = call(
                round_kernel, turn * lon * 60, turn * lon * held * 4,
                [smem, smem] + [vmem] * PLANES, [where, weights, *around],
                [near(held + SLOW + 1, turn, width)] * plane,
            )
            around = parts[:1] + [move(parts[shift], swaps[shift]) for shift in range(1, plane)]
        elif kind == "F":
            outs = finish(functools.partial(round_final_kernel, held, matrices), turn, around, outs)
        elif kind == "p":
            first, rows = firsts[at], sizes[at]
            parts = fetch(
                [near(PLANES, held, rows, width)] * 3,
                lambda w, first=first, rows=rows: [
                    (out, 0, first, rows, step, column(w, step, shift))
                    for out, shift in ((1, 2), (2, 3), (0, 0))
                    for step in range(PLANES)
                ],
                rows,
            )
            packed[at] = [parts[0], move(parts[1], swaps[2]), move(parts[2], swaps[3])]
        elif kind == "q":
            first, rows = firsts[PAIRS[at][0]], sum(sizes[chunk] for chunk in PAIRS[at])
            (part,) = fetch(
                [near(PLANES, held, rows, width)],
                lambda w, first=first, rows=rows: [(0, 0, first, rows, step, column(w, step, 1)) for step in range(PLANES)],
                rows,
            )
            part = move(part, swaps[1])
            for chunk in PAIRS[at]:
                paired[chunk] = (part, firsts[chunk] - first)
        elif kind == "t":
            rows = sizes[at]
            mode = next(mode for mode, chunks in GROUPS if at in chunks)
            part, offset = paired[at]
            home[at], own[at], far[at] = call(
                functools.partial(totals_kernel, offset), rows * width * PLANES * 240, rows * width * 656,
                [smem, smem] + [vmem] * plane, [where, weights, packed[at][0], part, *packed[at][1:]],
                [near(STATS, rows, width)] * 2 + [near(2, STATS, rows, width)],
            )
            moved["a", at] = move(far[at], to_inner)
            if mode == "e":
                moved["h", at] = move(home[at], to_outer)
        elif kind == "n":
            chunks = NEARS[at]
            rows = sum(sizes[chunk] for chunk in chunks)
            (part,) = call(
                functools.partial(join_kernel, len(chunks)), rows * width * 17, rows * width * 136,
                [vmem] * len(chunks), [own[chunk] for chunk in chunks], [near(STATS, rows, width)],
            )
            part = move(part, to_inner)
            for chunk in chunks:
                moved["n", chunk] = (part, sum(sizes[other] for other in chunks if other < chunk))
        elif kind == "m":
            mode, chunks = GROUPS[at]
            rows = sum(sizes[chunk] for chunk in chunks)
            shapes = [near(STATS, rows, width)] * 2 if mode == "e" else [near(2, STATS, rows, width)]
            args = [far[chunk] for chunk in chunks] + [moved["a", chunk] for chunk in chunks]
            parts = call(
                functools.partial(merge_kernel, len(chunks), mode == "e"), rows * width * 34, rows * width * 408,
                [vmem] * len(args), args, shapes,
            )
            moved["b", at] = move(parts[0], middle)
            if mode == "e":
                moved["g", at] = move(parts[1], across)
        elif kind == "r":
            chunks = GROUPS[at][1]
            rows = sum(sizes[chunk] for chunk in chunks)
            (part,) = call(
                functools.partial(relay_kernel, len(chunks)), rows * width * 17, rows * width * 204,
                [vmem] * (1 + len(chunks)), [moved["b", at]] + [home[chunk] for chunk in chunks],
                [near(STATS, rows, width)],
            )
            moved["c", at] = move(part, to_outer)
        else:
            mode, chunks = GROUPS[at]
            rows = sum(sizes[chunk] for chunk in chunks)
            args = [home[chunk] for chunk in chunks] + [own[chunk] for chunk in chunks]
            args += [moved["n", chunk][0] for chunk in chunks] + [moved["b", at]]
            args += [moved["g", at], moved["h", chunks[0]]] if mode == "e" else [moved["c", at]]
            places = [(sizes[chunk], moved["n", chunk][1]) for chunk in chunks]
            kernel = functools.partial(final_kernel, firsts[chunks[0]], places, mode, matrices)
            outs = finish(kernel, rows, args, outs)
    return tuple(outs)


def fits(groups):
    return groups == 4 * PLANES and TIMES % groups == 0 and TIMES // PLANES == 2 * PERIOD


def local(snapshots):
    groups = lax.axis_size("io")
    lat = snapshots.shape[0] * groups // TIMES
    if fits(groups) and lat % (8 * (ROUND + sum(PARTS))) == 0 and snapshots.shape[1] == 128 * groups:
        return plane_plan(snapshots)
    return general(snapshots)


def solution(mesh):
    return jax.shard_map(
        local,
        mesh=mesh,
        in_specs=(P(("rep", "io"), None),),
        out_specs=(P("rep", None, "io"), P("rep", "io")),
        check_vma=False,
    )
```

```python
import functools

import jax
import jax.numpy as jnp
import numpy as np
from jax import lax
from jax.experimental import pallas as pl
from jax.experimental.pallas import tpu as pltpu
from jax.sharding import PartitionSpec as P


TIMES = 96
HARM = 16
PERIOD = 12
SLOW = HARM - PERIOD
STATS = HARM + 1
PLANES = 4

ROUND = 4
PARTS = (6, 5, 4, 5, 4, 4)
GROUPS = (("s", (0, 1, 2)), ("s", (3, 4)), ("s", (5,)))
NEARS = ((2, 3, 4), (5,))
PAIRS = ((0, 1, 2, 3, 4, 5),)
ORDER = " ".join((
    "p0 P0 q0 p1",
    "p2 p3 t0 S0",
    "p4 p5 t1 m0",
    "t2 R0 m1 t3",
    "T0 m2 t4 m3",
    "r0 t5 m4 n0",
    "n1 F0 m5 r1",
    "r2 f0 f1 f2",
)).split()
FINAL_ROWS = 8
VMEM_LIMIT = 8 << 20


def basis_matrix(times):
    steps = np.arange(times, dtype=np.float64)
    columns = [np.ones_like(steps), (steps - (times - 1) / 2.0) / (times / 2.0)]
    for harmonic in range(1, 7):
        columns.append(np.cos(2.0 * np.pi * harmonic * steps / 12.0))
    for harmonic in range(1, 6):
        columns.append(np.sin(2.0 * np.pi * harmonic * steps / 12.0))
    columns.append(np.cos(2.0 * np.pi * steps / times))
    columns.append(np.sin(2.0 * np.pi * steps / times))
    columns.append(np.cos(4.0 * np.pi * steps / times))
    return np.stack(columns, axis=1)


PERIODIC = [0] + list(range(2, 13))
SLOWS = [1, 13, 14, 15]


def fit_matrices():
    basis = basis_matrix(TIMES)
    to_moments = np.zeros((HARM, HARM))
    for column in PERIODIC:
        to_moments[column, :PERIOD] = basis[:PERIOD, column]
    for at, column in enumerate(SLOWS):
        to_moments[column, PERIOD + at] = 1.0
    to_coeffs = np.linalg.solve(basis.T @ basis, to_moments)
    return to_moments, to_coeffs


def fit_block(block, basis, projector):
    width = block.shape[-1]
    lat_rows = block.shape[0] // TIMES
    series = block.reshape(TIMES, lat_rows * width)
    coeffs = jnp.dot(projector, series, precision=lax.Precision.HIGHEST)
    moments = jnp.dot(basis.T, series, precision=lax.Precision.HIGHEST)
    total = jnp.sum(series * series, axis=0)
    variance = (total - jnp.sum(coeffs * moments, axis=0)) / TIMES
    return coeffs.reshape(HARM, lat_rows, width), variance.reshape(lat_rows, width)


def general(snapshots):
    groups = lax.axis_size("io")
    local_rows = snapshots.shape[0]
    lon_dev = snapshots.shape[1] // groups
    split_view = snapshots.reshape(local_rows, groups, lon_dev)
    basis = basis_matrix(TIMES)
    projector = np.linalg.solve(basis.T @ basis, basis.T)
    moved = lax.all_to_all(split_view, "io", split_axis=1, concat_axis=0, tiled=True)
    return fit_block(moved[:, 0, :], jnp.float32(basis), jnp.float32(projector))


def fetch_kernel(pieces, where_ref, x_ref, *rest):
    outs, sem = rest[-1 - pieces(None) - 1 : -2], rest[-1]
    copies = []
    for out, to_rows, first, rows, at, column in pieces(where_ref):
        ref = outs[out] if at is None else outs[out].at[at]
        width = ref.shape[-1]
        source = x_ref.at[:, pl.ds(first, rows), pl.ds(pl.multiple_of(column, width), width)]
        copies.append(pltpu.make_async_copy(source, ref.at[:, pl.ds(to_rows, rows)], sem))
        copies[-1].start()
    for copy in copies:
        copy.wait()


def sums(values, weights, way, emit):
    slow, square = [None] * SLOW, None
    held = len(values[0])
    for k in range(held):
        for at, source in enumerate(values):
            for j in range(SLOW):
                term = source[k] * weights[way * SLOW + j, at * held + k]
                slow[j] = term if slow[j] is None else slow[j] + term
            term = source[k] * source[k]
            square = term if square is None else square + term
    for j in range(SLOW):
        emit(j, slow[j])
    emit(SLOW, square)


def row_blocks(rows, body):
    size = 16 if rows % 16 == 0 else 8

    @pl.loop(0, rows // size)
    def _(block):
        body(block * size, size)


def totals_kernel(offset, split, where_ref, weight_ref, own_ref, r1_ref, r2_ref, r3_ref, *rest):
    home_ref, near_ref, far_ref = rest[-4:-1] if split else (rest[-3], None, rest[-2])
    held, rows = own_ref.shape[1:3]
    first = (where_ref[0] % 2) * held
    second = held - first
    for step in range(PLANES):
        out_ref = (home_ref, near_ref if near_ref is not None else far_ref.at[2], far_ref.at[0], far_ref.at[1])[step]

        def body(start, size):
            at, at1 = pl.ds(pl.multiple_of(start, 8), size), pl.ds(pl.multiple_of(start + offset, 8), size)
            values = [
                [ref[step, k, rows_] for k in range(held)]
                for ref, rows_ in ((own_ref, at), (r1_ref, at1), (r2_ref, at), (r3_ref, at))
            ]
            for k in range(held):
                out_ref[first + k, at] = values[0][k] + values[2][k]
                out_ref[second + k, at] = values[1][k] + values[3][k]

            def emit(row, value):
                out_ref[PERIOD + row, at] = value

            sums(values, weight_ref, 0, emit)

        row_blocks(rows, body)


def round_sums_kernel(where_ref, weight_ref, own_ref, in_ref, *rest):
    home_ref, near_ref, far_ref = rest[-4:-1]
    held, rows = own_ref.shape[1:3]
    width = 128
    for step in range(PLANES):
        out_ref = (home_ref, near_ref, far_ref.at[0], far_ref.at[1])[step]
        for part in range(own_ref.shape[3] // width):
            columns = slice(part * width, (part + 1) * width)

            def body(start, size):
                at = pl.ds(pl.multiple_of(start, 8), size)
                values = [[own_ref[step, k, at, columns] for k in range(held)]]
                if step > 0:
                    values.append([in_ref[step - 1, k, at, columns] for k in range(held)])
                for k in range(held):
                    out_ref[k, at, columns] = values[0][k] + values[1][k] if step > 0 else values[0][k]

                def emit(row, value):
                    out_ref[held + row, at, columns] = value

                sums(values, weight_ref, 1, emit)

            row_blocks(rows, body)


def round_relay_kernel(home_ref, b_ref, *rest):
    rest[-2][...] = home_ref[...] + b_ref[1]


def round_split_kernel(where_ref, home_ref, near_ref, b_ref, c_ref, *rest):
    outs = rest[-5:-1]
    width = outs[0].shape[-1]
    for shift, out_ref in enumerate(outs):
        column = pl.ds(pl.multiple_of((where_ref[0] ^ shift) * width, width), width)

        @pl.when(where_ref[1] > 0)
        def _():
            out_ref[...] = near_ref[:, :, column] + b_ref[0, :, :, column]

        @pl.when(where_ref[1] == 0)
        def _():
            out_ref[...] = home_ref[:, :, column] + c_ref[:, :, column]


def join_kernel(count, *refs):
    out_ref, start = refs[-2], 0
    for ref in refs[:count]:
        rows = ref.shape[1]
        out_ref[:, start : start + rows] = ref[...]
        start += rows


def merge_kernel(straight, own_ref, in_ref, *rest):
    outs = rest[-3:-1] if straight else rest[-2:-1]
    for hop in range(2):
        out_ref = outs[hop] if straight else outs[0].at[hop]
        out_ref[...] = own_ref[hop] + in_ref[hop]


def relay_kernel(count, *refs):
    out_ref, start = refs[-2], 0
    for home_ref, b_ref in zip(refs[:count], refs[count : 2 * count]):
        rows = home_ref.shape[1]
        out_ref[:, start : start + rows] = home_ref[...] + b_ref[1]
        start += rows


def solve(matrices, coeff_ref, var_ref, start, rows, load):
    to_moments, to_coeffs = matrices

    @pl.loop(0, rows // FINAL_ROWS)
    def _(block):
        at = pl.multiple_of(block * FINAL_ROWS, FINAL_ROWS)
        stats = [load(row, at) for row in range(STATS)]

        def mix(weights):
            total = None
            for weight, stat in zip(weights, stats):
                if abs(weight) > 1e-12:
                    term = stat if weight == 1.0 else stat * np.float32(weight)
                    total = term if total is None else total + term
            return total

        to = pl.ds(pl.multiple_of(start + at, FINAL_ROWS), FINAL_ROWS)
        explained = None
        for column in range(HARM):
            coeff = mix(to_coeffs[column])
            coeff_ref[column, to] = coeff
            term = coeff * mix(to_moments[column])
            explained = term if explained is None else explained + term
        var_ref[to] = (stats[HARM] - explained) * np.float32(1.0 / TIMES)


def store(first, coeff_out, var_out, coeff_ref, var_ref, sem):
    rows = var_ref.shape[0]
    copies = [
        pltpu.make_async_copy(coeff_ref, coeff_out.at[:, pl.ds(first, rows)], sem.at[0]),
        pltpu.make_async_copy(var_ref, var_out.at[pl.ds(first, rows)], sem.at[1]),
    ]
    for copy in copies:
        copy.start()
    for copy in copies:
        copy.wait()


def final_kernel(first, chunks, mode, matrices, where_ref, *refs):
    coeff_out, var_out, _, coeff_ref, var_ref, sem = refs[-6:]
    count = len(chunks)
    homes, owns, nears = refs[:count], refs[count : 2 * count], refs[2 * count : 3 * count]
    middles, two_ref = refs[3 * count : 4 * count], refs[4 * count]

    @pl.when(where_ref[1] > 0)
    def _():
        start = 0
        for (rows, place), own_ref, in_ref, b_ref in zip(chunks, owns, nears, middles):

            def load(row, at, place=place, own_ref=own_ref, in_ref=in_ref, b_ref=b_ref):
                middle = b_ref if mode == "e" else b_ref.at[0]
                own_part, in_part = (ref if len(ref.shape) == 3 else ref.at[2] for ref in (own_ref, in_ref))
                value = own_part[row, pl.ds(at, FINAL_ROWS)] + in_part[row, pl.ds(pl.multiple_of(at + place, 8), FINAL_ROWS)]
                return value + middle[row, pl.ds(at, FINAL_ROWS)]

            solve(matrices, coeff_ref, var_ref, start, rows, load)
            start += rows

    @pl.when(where_ref[1] == 0)
    def _():
        start = 0
        for (rows, place), home_ref in zip(chunks, homes):

            def load(row, at, start=start, home_ref=home_ref):
                value = home_ref[row, pl.ds(at, FINAL_ROWS)] + two_ref[row, pl.ds(pl.multiple_of(at + start, 8), FINAL_ROWS)]
                if mode == "e":
                    value = value + refs[4 * count + 1][row, pl.ds(at, FINAL_ROWS)]
                return value

            solve(matrices, coeff_ref, var_ref, start, rows, load)
            start += rows

    store(first, coeff_out, var_out, coeff_ref, var_ref, sem)


def round_final_kernel(held, matrices, where_ref, *refs):
    coeff_out, var_out, _, coeff_ref, var_ref, sem = refs[-6:]
    rows = var_ref.shape[0]

    def run(early, late):
        def load(row, at):
            rows_ = pl.ds(at, FINAL_ROWS)
            if row < PERIOD:
                one, two = early if row < held else late
                return one[row % held, rows_] + two[row % held, rows_]
            row = row - PERIOD + held
            return (refs[0][row, rows_] + refs[1][row, rows_]) + (refs[2][row, rows_] + refs[3][row, rows_])

        solve(matrices, coeff_ref, var_ref, 0, rows, load)

    @pl.when(where_ref[0] % 2 == 0)
    def _():
        run((refs[0], refs[2]), (refs[1], refs[3]))

    @pl.when(where_ref[0] % 2 == 1)
    def _():
        run((refs[1], refs[3]), (refs[0], refs[2]))

    store(0, coeff_out, var_out, coeff_ref, var_ref, sem)


def plane_plan(snapshots):
    groups = lax.axis_size("io")
    plane = groups // PLANES
    held = TIMES // groups
    lat = snapshots.shape[0] // held
    lon = snapshots.shape[1]
    width = lon // groups
    view = snapshots.reshape(held, lat, lon)

    me = lax.axis_index("io")
    place, level = me % plane, me // plane
    flip = (level >= PLANES // 2).astype(jnp.int32)
    inner = ((level > 0) & (level < PLANES - 1)).astype(jnp.int32)
    where = jnp.stack([place, inner, flip, level]).astype(jnp.int32)

    slow = basis_matrix(TIMES)[:, SLOWS].T
    table = np.zeros((groups, 2 * SLOW, plane * held), np.float32)
    for device in range(groups):
        for shift in range(plane):
            for way, other in enumerate((device ^ shift, device ^ (shift * plane))):
                rows, columns = way * SLOW, shift * held
                table[device, rows : rows + SLOW, columns : columns + held] = slow[:, other * held : (other + 1) * held]
    weights = lax.dynamic_index_in_dim(jnp.asarray(table), me, 0, keepdims=False)
    matrices = fit_matrices()

    smem = pl.BlockSpec(memory_space=pltpu.SMEM)
    vmem = pl.BlockSpec(memory_space=pltpu.VMEM)
    hbm = pl.BlockSpec(memory_space=pltpu.HBM)
    space = {id(vmem): pltpu.VMEM, id(hbm): pltpu.HBM}
    token = [weights]

    def near(*dims):
        return pltpu.VMEM(dims, jnp.float32)

    def call(kernel, flops, moved, ins, args, outs, out_specs=None, **more):
        ins, args = ins + [hbm] * len(token), list(args) + token
        args = [
            pltpu.with_memory_space_constraint(arg, space[id(spec)]) if id(spec) in space else arg
            for spec, arg in zip(ins, args)
        ]
        *results, last = pl.pallas_call(
            kernel,
            in_specs=ins,
            out_specs=(out_specs or [vmem] * len(outs)) + [hbm],
            out_shape=outs + [pltpu.HBM((8, 128), jnp.float32)],
            cost_estimate=pl.CostEstimate(flops=flops, bytes_accessed=moved, transcendentals=0),
            compiler_params=pltpu.CompilerParams(vmem_limit_bytes=VMEM_LIMIT),
            **more,
        )(*args)
        token[:] = [last]
        return results

    def move(value, pairs):
        return lax.ppermute(value, "io", pairs)

    unit = lat // (ROUND + sum(PARTS))
    sizes = [part * unit for part in PARTS]
    firsts = [(ROUND + sum(PARTS[:chunk])) * unit for chunk in range(len(PARTS))]
    turn = ROUND * unit
    swaps = [[(i, i ^ shift) for i in range(groups)] for shift in range(plane)]
    to_inner = [(i, i + plane) for i in range(plane)] + [(i, i - plane) for i in range(groups - plane, groups)]
    to_outer = [(b, a) for a, b in to_inner]
    middle = [(i, i + plane) for i in range(plane, 2 * plane)]
    middle = middle + [(b, a) for a, b in middle]
    across = [(i, i + 2 * plane) for i in range(plane, 2 * plane)]
    across = across + [(i, i - 2 * plane) for i in range(2 * plane, 3 * plane)]

    def fetch(outs, pieces, rows):
        def count_or_pieces(where_ref):
            return len(outs) if where_ref is None else pieces(where_ref)

        return call(
            functools.partial(fetch_kernel, count_or_pieces), rows * lon, rows * lon * held * 8,
            [smem, hbm], [where, view], outs, scratch_shapes=[pltpu.SemaphoreType.DMA],
        )

    def column(where_ref, step, shift):
        zone = jnp.where(where_ref[2] > 0, PLANES - 1 - step, step)
        return (zone * plane + (where_ref[0] ^ shift)) * width

    def finish(kernel, rows, args, outs):
        count = len(args)
        return call(
            kernel, rows * width * 832, rows * width * 272,
            [smem] + [vmem] * count + [hbm] * len(outs), [where, *args, *outs],
            [pltpu.HBM((HARM, lat, width), jnp.float32), pltpu.HBM((lat, width), jnp.float32)], [hbm, hbm],
            input_output_aliases={count + 1: 0, count + 2: 1} if outs else {},
            scratch_shapes=[
                pltpu.VMEM((HARM, rows, width), jnp.float32),
                pltpu.VMEM((rows, width), jnp.float32),
                pltpu.SemaphoreType.DMA((2,)),
            ],
        )

    packed, paired, home, own, far, moved, outs = {}, {}, {}, {}, {}, {}, []
    for item in ORDER:
        kind, at = item[0], int(item[1:])
        if kind == "P":
            parts = fetch(
                [near(PLANES, held, turn, plane * width), near(PLANES - 1, held, turn, plane * width)],
                lambda w: [
                    (out, 0, 0, turn, step - out, column(w, step, w[0]))
                    for out, steps in ((1, (1, 2, 3)), (0, range(PLANES)))
                    for step in steps
                ],
                turn,
            )
            around = [parts[0], move(parts[1], to_inner)]
        elif kind == "S":
            parts = call(
                round_sums_kernel, turn * lon * 40, turn * lon * held * 8,
                [smem, smem, vmem, vmem], [where, weights, *around],
                [near(held + SLOW + 1, turn, plane * width)] * 2 + [near(2, held + SLOW + 1, turn, plane * width)],
            )
            around = [parts[0], parts[1], move(parts[2], middle)]
        elif kind == "R":
            (part,) = call(
                round_relay_kernel, turn * lon, turn * lon * 12,
                [vmem, vmem], [around[0], around[2]], [near(held + SLOW + 1, turn, plane * width)],
            )
            around.append(move(part, to_outer))
        elif kind == "T":
            parts = call(
                round_split_kernel, turn * lon, turn * lon * 12,
                [smem] + [vmem] * 4, [where, *around],
                [near(held + SLOW + 1, turn, width)] * plane,
            )
            around = parts[:1] + [move(parts[shift], swaps[shift]) for shift in range(1, plane)]
        elif kind == "F":
            outs = finish(functools.partial(round_final_kernel, held, matrices), turn, around, outs)
        elif kind == "p":
            first, rows = firsts[at], sizes[at]
            parts = fetch(
                [near(PLANES, held, rows, width)] * 3,
                lambda w, first=first, rows=rows: [
                    (out, 0, first, rows, step, column(w, step, shift))
                    for out, shift in ((1, 2), (2, 3), (0, 0))
                    for step in range(PLANES)
                ],
                rows,
            )
            packed[at] = [parts[0], move(parts[1], swaps[2]), move(parts[2], swaps[3])]
        elif kind == "q":
            first, rows = firsts[PAIRS[at][0]], sum(sizes[chunk] for chunk in PAIRS[at])
            (part,) = fetch(
                [near(PLANES, held, rows, width)],
                lambda w, first=first, rows=rows: [(0, 0, first, rows, step, column(w, step, 1)) for step in range(PLANES)],
                rows,
            )
            part = move(part, swaps[1])
            for chunk in PAIRS[at]:
                paired[chunk] = (part, firsts[chunk] - first)
        elif kind == "t":
            rows = sizes[at]
            mode = next(mode for mode, chunks in GROUPS if at in chunks)
            part, offset = paired[at]
            split = any(at in chunks for chunks in NEARS)
            results = call(
                functools.partial(totals_kernel, offset, split), rows * width * PLANES * 240, rows * width * 656,
                [smem, smem] + [vmem] * plane, [where, weights, packed[at][0], part, *packed[at][1:]],
                [near(STATS, rows, width)] * (2 if split else 1) + [near(2 if split else 3, STATS, rows, width)],
            )
            home[at], own[at], far[at] = results[0], results[-2] if split else results[-1], results[-1]
            moved["a", at] = move(far[at], to_inner)
            if not split:
                moved["n", at] = (moved["a", at], 0)
            if mode == "e":
                moved["h", at] = move(home[at], to_outer)
        elif kind == "n":
            chunks = NEARS[at]
            rows = sum(sizes[chunk] for chunk in chunks)
            (part,) = call(
                functools.partial(join_kernel, len(chunks)), rows * width * 17, rows * width * 136,
                [vmem] * len(chunks), [own[chunk] for chunk in chunks], [near(STATS, rows, width)],
            )
            part = move(part, to_inner)
            for chunk in chunks:
                moved["n", chunk] = (part, sum(sizes[other] for other in chunks if other < chunk))
        elif kind == "m":
            rows = sizes[at]
            mode = next(mode for mode, chunks in GROUPS if at in chunks)
            parts = call(
                functools.partial(merge_kernel, mode == "e"), rows * width * 34, rows * width * 408,
                [vmem] * 2, [far[at], moved["a", at]],
                [near(STATS, rows, width)] * 2 if mode == "e" else [near(2, STATS, rows, width)],
            )
            moved["b", at] = move(parts[0], middle)
            if mode == "e":
                moved["g", at] = move(parts[1], across)
        elif kind == "r":
            chunks = GROUPS[at][1]
            rows = sum(sizes[chunk] for chunk in chunks)
            args = [home[chunk] for chunk in chunks] + [moved["b", chunk] for chunk in chunks]
            (part,) = call(
                functools.partial(relay_kernel, len(chunks)), rows * width * 17, rows * width * 204,
                [vmem] * len(args), args, [near(STATS, rows, width)],
            )
            moved["c", at] = move(part, to_outer)
        else:
            mode, chunks = GROUPS[at]
            rows = sum(sizes[chunk] for chunk in chunks)
            args = [home[chunk] for chunk in chunks] + [own[chunk] for chunk in chunks]
            args += [moved["n", chunk][0] for chunk in chunks] + [moved["b", chunk] for chunk in chunks]
            args += [moved["g", chunks[0]], moved["h", chunks[0]]] if mode == "e" else [moved["c", at]]
            places = [(sizes[chunk], moved["n", chunk][1]) for chunk in chunks]
            kernel = functools.partial(final_kernel, firsts[chunks[0]], places, mode, matrices)
            outs = finish(kernel, rows, args, outs)
    return tuple(outs)


def fits(groups):
    return groups == 4 * PLANES and TIMES % groups == 0 and TIMES // PLANES == 2 * PERIOD


def local(snapshots):
    groups = lax.axis_size("io")
    lat = snapshots.shape[0] * groups // TIMES
    if fits(groups) and lat % (8 * (ROUND + sum(PARTS))) == 0 and snapshots.shape[1] == 128 * groups:
        return plane_plan(snapshots)
    return general(snapshots)


def solution(mesh):
    return jax.shard_map(
        local,
        mesh=mesh,
        in_specs=(P(("rep", "io"), None),),
        out_specs=(P("rep", None, "io"), P("rep", "io")),
        check_vma=False,
    )
```

```python
import functools

import jax
import jax.numpy as jnp
import numpy as np
from jax import lax
from jax.experimental import pallas as pl
from jax.experimental.pallas import tpu as pltpu
from jax.sharding import PartitionSpec as P


TIMES = 96
HARM = 16
PERIOD = 12
SLOW = HARM - PERIOD
STATS = HARM + 1
PLANES = 4

ROUND = 4
PARTS = (4, 4, 5, 2, 4, 4, 3, 2)
GROUPS = (("s", (0, 1, 2)), ("s", (3, 4)), ("s", (5,)), ("s", (6,)), ("s", (7,)))
NEARS = ((4, 5, 6), (7,))
ORDER = " ".join((
    "P0 q0 p1 p2",
    "p3 t0 S0 p4",
    "t1 p5 m0 p6",
    "p7 t2 m1 R0",
    "t3 T0 m2 t4",
    "m3 t5 r0 m4",
    "t6 m5 t7 r1",
    "n0 m6 F0 m7",
    "r2 f0 n1 r3",
    "f1 r4 f2 f3",
    "f4",
)).split()
FINAL_ROWS = 8
VMEM_LIMIT = 8 << 20


def basis_matrix(times):
    steps = np.arange(times, dtype=np.float64)
    columns = [np.ones_like(steps), (steps - (times - 1) / 2.0) / (times / 2.0)]
    for harmonic in range(1, 7):
        columns.append(np.cos(2.0 * np.pi * harmonic * steps / 12.0))
    for harmonic in range(1, 6):
        columns.append(np.sin(2.0 * np.pi * harmonic * steps / 12.0))
    columns.append(np.cos(2.0 * np.pi * steps / times))
    columns.append(np.sin(2.0 * np.pi * steps / times))
    columns.append(np.cos(4.0 * np.pi * steps / times))
    return np.stack(columns, axis=1)


PERIODIC = [0] + list(range(2, 13))
SLOWS = [1, 13, 14, 15]


def fit_matrices():
    basis = basis_matrix(TIMES)
    to_moments = np.zeros((HARM, HARM))
    for column in PERIODIC:
        to_moments[column, :PERIOD] = basis[:PERIOD, column]
    for at, column in enumerate(SLOWS):
        to_moments[column, PERIOD + at] = 1.0
    to_coeffs = np.linalg.solve(basis.T @ basis, to_moments)
    return to_moments, to_coeffs


def fit_block(block, basis, projector):
    width = block.shape[-1]
    lat_rows = block.shape[0] // TIMES
    series = block.reshape(TIMES, lat_rows * width)
    coeffs = jnp.dot(projector, series, precision=lax.Precision.HIGHEST)
    moments = jnp.dot(basis.T, series, precision=lax.Precision.HIGHEST)
    total = jnp.sum(series * series, axis=0)
    variance = (total - jnp.sum(coeffs * moments, axis=0)) / TIMES
    return coeffs.reshape(HARM, lat_rows, width), variance.reshape(lat_rows, width)


def general(snapshots):
    groups = lax.axis_size("io")
    local_rows = snapshots.shape[0]
    lon_dev = snapshots.shape[1] // groups
    split_view = snapshots.reshape(local_rows, groups, lon_dev)
    basis = basis_matrix(TIMES)
    projector = np.linalg.solve(basis.T @ basis, basis.T)
    moved = lax.all_to_all(split_view, "io", split_axis=1, concat_axis=0, tiled=True)
    return fit_block(moved[:, 0, :], jnp.float32(basis), jnp.float32(projector))


def fetch_kernel(pieces, where_ref, x_ref, table_ref, *rest):
    count, with_table = pieces(None)
    outs, sem = rest[-2 - count : -2], rest[-1]
    copies = []
    if with_table:
        copies.append(pltpu.make_async_copy(table_ref.at[where_ref[3] * 4 + where_ref[0]], outs[-1], sem))
        copies[0].start()
    for out, to_rows, first, rows, at, column in pieces(where_ref):
        ref = outs[out] if at is None else outs[out].at[at]
        width = ref.shape[-1]
        source = x_ref.at[:, pl.ds(first, rows), pl.ds(pl.multiple_of(column, width), width)]
        copies.append(pltpu.make_async_copy(source, ref.at[:, pl.ds(to_rows, rows)], sem))
        copies[-1].start()
    for copy in copies:
        copy.wait()


def sums(values, weights, way, emit):
    slow, square = [None] * SLOW, None
    held = len(values[0])
    for k in range(held):
        for at, source in enumerate(values):
            for j in range(SLOW):
                term = source[k] * weights[way * SLOW + j, at * held + k]
                slow[j] = term if slow[j] is None else slow[j] + term
            term = source[k] * source[k]
            square = term if square is None else square + term
    for j in range(SLOW):
        emit(j, slow[j])
    emit(SLOW, square)


def row_blocks(rows, body):
    size = 16 if rows % 16 == 0 else 8

    @pl.loop(0, rows // size)
    def _(block):
        body(block * size, size)


def totals_kernel(offset, split, where_ref, weight_ref, own_ref, r1_ref, r2_ref, r3_ref, *rest):
    home_ref, near_ref, far_ref = rest[-4:-1] if split else (rest[-3], None, rest[-2])
    held, rows = own_ref.shape[1:3]
    first = (where_ref[0] % 2) * held
    second = held - first
    for step in range(PLANES):
        out_ref = (home_ref, near_ref if near_ref is not None else far_ref.at[2], far_ref.at[0], far_ref.at[1])[step]

        def body(start, size):
            at, at1 = pl.ds(pl.multiple_of(start, 8), size), pl.ds(pl.multiple_of(start + offset, 8), size)
            values = [
                [ref[step, k, rows_] for k in range(held)]
                for ref, rows_ in ((own_ref, at), (r1_ref, at1), (r2_ref, at), (r3_ref, at))
            ]
            for k in range(held):
                out_ref[first + k, at] = values[0][k] + values[2][k]
                out_ref[second + k, at] = values[1][k] + values[3][k]

            def emit(row, value):
                out_ref[PERIOD + row, at] = value

            sums(values, weight_ref, 0, emit)

        row_blocks(rows, body)


def round_sums_kernel(where_ref, weight_ref, own_ref, in_ref, *rest):
    home_ref, near_ref, far_ref = rest[-4:-1]
    held, rows = own_ref.shape[1:3]
    width = 128
    for step in range(PLANES):
        out_ref = (home_ref, near_ref, far_ref.at[0], far_ref.at[1])[step]
        for part in range(own_ref.shape[3] // width):
            columns = slice(part * width, (part + 1) * width)

            def body(start, size):
                at = pl.ds(pl.multiple_of(start, 8), size)
                values = [[own_ref[step, k, at, columns] for k in range(held)]]
                if step > 0:
                    values.append([in_ref[step - 1, k, at, columns] for k in range(held)])
                for k in range(held):
                    out_ref[k, at, columns] = values[0][k] + values[1][k] if step > 0 else values[0][k]

                def emit(row, value):
                    out_ref[held + row, at, columns] = value

                sums(values, weight_ref, 1, emit)

            row_blocks(rows, body)


def round_relay_kernel(home_ref, b_ref, *rest):
    rest[-2][...] = home_ref[...] + b_ref[1]


def round_split_kernel(where_ref, home_ref, near_ref, b_ref, c_ref, *rest):
    outs = rest[-5:-1]
    width = outs[0].shape[-1]
    for shift, out_ref in enumerate(outs):
        column = pl.ds(pl.multiple_of((where_ref[0] ^ shift) * width, width), width)

        @pl.when(where_ref[1] > 0)
        def _():
            out_ref[...] = near_ref[:, :, column] + b_ref[0, :, :, column]

        @pl.when(where_ref[1] == 0)
        def _():
            out_ref[...] = home_ref[:, :, column] + c_ref[:, :, column]


def join_kernel(count, *refs):
    out_ref, start = refs[-2], 0
    for ref in refs[:count]:
        rows = ref.shape[1]
        out_ref[:, start : start + rows] = ref[...]
        start += rows


def merge_kernel(straight, own_ref, in_ref, *rest):
    outs = rest[-3:-1] if straight else rest[-2:-1]
    for hop in range(2):
        out_ref = outs[hop] if straight else outs[0].at[hop]
        out_ref[...] = own_ref[hop] + in_ref[hop]


def relay_kernel(count, *refs):
    out_ref, start = refs[-2], 0
    for home_ref, b_ref in zip(refs[:count], refs[count : 2 * count]):
        rows = home_ref.shape[1]
        out_ref[:, start : start + rows] = home_ref[...] + b_ref[1]
        start += rows


def solve(matrices, coeff_ref, var_ref, start, rows, load):
    to_moments, to_coeffs = matrices

    @pl.loop(0, rows // FINAL_ROWS)
    def _(block):
        at = pl.multiple_of(block * FINAL_ROWS, FINAL_ROWS)
        stats = [load(row, at) for row in range(STATS)]

        def mix(weights):
            total = None
            for weight, stat in zip(weights, stats):
                if abs(weight) > 1e-12:
                    term = stat if weight == 1.0 else stat * np.float32(weight)
                    total = term if total is None else total + term
            return total

        to = pl.ds(pl.multiple_of(start + at, FINAL_ROWS), FINAL_ROWS)
        explained = None
        for column in range(HARM):
            coeff = mix(to_coeffs[column])
            coeff_ref[column, to] = coeff
            term = coeff * mix(to_moments[column])
            explained = term if explained is None else explained + term
        var_ref[to] = (stats[HARM] - explained) * np.float32(1.0 / TIMES)


def store(first, coeff_out, var_out, coeff_ref, var_ref, sem):
    rows = var_ref.shape[0]
    copies = [
        pltpu.make_async_copy(coeff_ref, coeff_out.at[:, pl.ds(first, rows)], sem.at[0]),
        pltpu.make_async_copy(var_ref, var_out.at[pl.ds(first, rows)], sem.at[1]),
    ]
    for copy in copies:
        copy.start()
    for copy in copies:
        copy.wait()


def final_kernel(first, chunks, mode, matrices, where_ref, *refs):
    coeff_out, var_out, _, coeff_ref, var_ref, sem = refs[-6:]
    count = len(chunks)
    homes, owns, nears = refs[:count], refs[count : 2 * count], refs[2 * count : 3 * count]
    middles, two_ref = refs[3 * count : 4 * count], refs[4 * count]

    @pl.when(where_ref[1] > 0)
    def _():
        start = 0
        for (rows, place), own_ref, in_ref, b_ref in zip(chunks, owns, nears, middles):

            def load(row, at, place=place, own_ref=own_ref, in_ref=in_ref, b_ref=b_ref):
                middle = b_ref if mode == "e" else b_ref.at[0]
                own_part, in_part = (ref if len(ref.shape) == 3 else ref.at[2] for ref in (own_ref, in_ref))
                value = own_part[row, pl.ds(at, FINAL_ROWS)] + in_part[row, pl.ds(pl.multiple_of(at + place, 8), FINAL_ROWS)]
                return value + middle[row, pl.ds(at, FINAL_ROWS)]

            solve(matrices, coeff_ref, var_ref, start, rows, load)
            start += rows

    @pl.when(where_ref[1] == 0)
    def _():
        start = 0
        for (rows, place), home_ref in zip(chunks, homes):

            def load(row, at, start=start, home_ref=home_ref):
                value = home_ref[row, pl.ds(at, FINAL_ROWS)] + two_ref[row, pl.ds(pl.multiple_of(at + start, 8), FINAL_ROWS)]
                if mode == "e":
                    value = value + refs[4 * count + 1][row, pl.ds(at, FINAL_ROWS)]
                return value

            solve(matrices, coeff_ref, var_ref, start, rows, load)
            start += rows

    store(first, coeff_out, var_out, coeff_ref, var_ref, sem)


def round_final_kernel(held, matrices, where_ref, *refs):
    coeff_out, var_out, _, coeff_ref, var_ref, sem = refs[-6:]
    rows = var_ref.shape[0]

    def run(early, late):
        def load(row, at):
            rows_ = pl.ds(at, FINAL_ROWS)
            if row < PERIOD:
                one, two = early if row < held else late
                return one[row % held, rows_] + two[row % held, rows_]
            row = row - PERIOD + held
            return (refs[0][row, rows_] + refs[1][row, rows_]) + (refs[2][row, rows_] + refs[3][row, rows_])

        solve(matrices, coeff_ref, var_ref, 0, rows, load)

    @pl.when(where_ref[0] % 2 == 0)
    def _():
        run((refs[0], refs[2]), (refs[1], refs[3]))

    @pl.when(where_ref[0] % 2 == 1)
    def _():
        run((refs[1], refs[3]), (refs[0], refs[2]))

    store(0, coeff_out, var_out, coeff_ref, var_ref, sem)


def plane_plan(snapshots):
    groups = lax.axis_size("io")
    plane = groups // PLANES
    held = TIMES // groups
    lat = snapshots.shape[0] // held
    lon = snapshots.shape[1]
    width = lon // groups
    view = snapshots.reshape(held, lat, lon)

    me = lax.axis_index("io")
    place, level = me % plane, me // plane
    flip = (level >= PLANES // 2).astype(jnp.int32)
    inner = ((level > 0) & (level < PLANES - 1)).astype(jnp.int32)
    where = jnp.stack([place, inner, flip, level]).astype(jnp.int32)

    slow = basis_matrix(TIMES)[:, SLOWS].T
    table = np.zeros((groups, 2 * SLOW, plane * held), np.float32)
    for device in range(groups):
        for shift in range(plane):
            for way, other in enumerate((device ^ shift, device ^ (shift * plane))):
                rows, columns = way * SLOW, shift * held
                table[device, rows : rows + SLOW, columns : columns + held] = slow[:, other * held : (other + 1) * held]
    table = jnp.asarray(table)
    matrices = fit_matrices()

    smem = pl.BlockSpec(memory_space=pltpu.SMEM)
    vmem = pl.BlockSpec(memory_space=pltpu.VMEM)
    hbm = pl.BlockSpec(memory_space=pltpu.HBM)
    space = {id(vmem): pltpu.VMEM, id(hbm): pltpu.HBM}
    token = []

    def near(*dims):
        return pltpu.VMEM(dims, jnp.float32)

    def call(kernel, flops, moved, ins, args, outs, out_specs=None, **more):
        ins, args = ins + [hbm] * len(token), list(args) + token
        args = [
            pltpu.with_memory_space_constraint(arg, space[id(spec)]) if id(spec) in space else arg
            for spec, arg in zip(ins, args)
        ]
        *results, last = pl.pallas_call(
            kernel,
            in_specs=ins,
            out_specs=(out_specs or [vmem] * len(outs)) + [hbm],
            out_shape=outs + [pltpu.HBM((8, 128), jnp.float32)],
            cost_estimate=pl.CostEstimate(flops=flops, bytes_accessed=moved, transcendentals=0),
            compiler_params=pltpu.CompilerParams(vmem_limit_bytes=VMEM_LIMIT),
            **more,
        )(*args)
        token[:] = [last]
        return results

    def move(value, pairs):
        return lax.ppermute(value, "io", pairs)

    unit = lat // (ROUND + sum(PARTS))
    sizes = [part * unit for part in PARTS]
    firsts = [(ROUND + sum(PARTS[:chunk])) * unit for chunk in range(len(PARTS))]
    turn = ROUND * unit
    swaps = [[(i, i ^ shift) for i in range(groups)] for shift in range(plane)]
    to_inner = [(i, i + plane) for i in range(plane)] + [(i, i - plane) for i in range(groups - plane, groups)]
    to_outer = [(b, a) for a, b in to_inner]
    middle = [(i, i + plane) for i in range(plane, 2 * plane)]
    middle = middle + [(b, a) for a, b in middle]
    across = [(i, i + 2 * plane) for i in range(plane, 2 * plane)]
    across = across + [(i, i - 2 * plane) for i in range(2 * plane, 3 * plane)]

    def fetch(outs, pieces, rows, with_table=False):
        outs = outs + [near(2 * SLOW, plane * held)] * with_table

        def count_or_pieces(where_ref):
            return (len(outs), with_table) if where_ref is None else pieces(where_ref)

        return call(
            functools.partial(fetch_kernel, count_or_pieces), rows * lon, rows * lon * held * 8,
            [smem, hbm, hbm], [where, view, table], outs, scratch_shapes=[pltpu.SemaphoreType.DMA],
        )

    def pieces_of(w, out, first, rows, shift):
        return [(out, 0, first, rows, step, column(w, step, shift)) for step in range(PLANES)]

    def column(where_ref, step, shift):
        zone = jnp.where(where_ref[2] > 0, PLANES - 1 - step, step)
        return (zone * plane + (where_ref[0] ^ shift)) * width

    def finish(kernel, rows, args, outs):
        count = len(args)
        return call(
            kernel, rows * width * 832, rows * width * 272,
            [smem] + [vmem] * count + [hbm] * len(outs), [where, *args, *outs],
            [pltpu.HBM((HARM, lat, width), jnp.float32), pltpu.HBM((lat, width), jnp.float32)], [hbm, hbm],
            input_output_aliases={count + 1: 0, count + 2: 1} if outs else {},
            scratch_shapes=[
                pltpu.VMEM((HARM, rows, width), jnp.float32),
                pltpu.VMEM((rows, width), jnp.float32),
                pltpu.SemaphoreType.DMA((2,)),
            ],
        )

    packed, home, own, far, moved, outs = {}, {}, {}, {}, {}, []
    for item in ORDER:
        kind, at = item[0], int(item[1:])
        if kind == "P":
            first, rows = firsts[0], sizes[0]
            parts = fetch(
                [near(PLANES - 1, held, turn, plane * width)] + [near(PLANES, held, rows, width)] * 2,
                lambda w: [(0, 0, 0, turn, step - 1, column(w, step, w[0])) for step in (1, 2, 3)]
                + pieces_of(w, 1, first, rows, 2) + pieces_of(w, 2, first, rows, 3),
                turn + rows,
            )
            around = [None, move(parts[0], to_inner)]
            packed[0] = [None, move(parts[1], swaps[2]), move(parts[2], swaps[3])]
        elif kind == "q":
            first, rows, own_rows = firsts[0], sum(sizes), sizes[0]
            parts = fetch(
                [near(PLANES, held, rows, width), near(PLANES, held, turn, plane * width), near(PLANES, held, own_rows, width)],
                lambda w: pieces_of(w, 0, first, rows, 1)
                + [(1, 0, 0, turn, step, column(w, step, w[0])) for step in range(PLANES)]
                + pieces_of(w, 2, first, own_rows, 0),
                rows, True,
            )
            part = move(parts[0], swaps[1])
            around[0], packed[0][0], weights = parts[1], parts[2], parts[3]
            paired = [(part, other - first) for other in firsts]
        elif kind == "S":
            parts = call(
                round_sums_kernel, turn * lon * 40, turn * lon * held * 8,
                [smem, smem, vmem, vmem], [where, weights, *around],
                [near(held + SLOW + 1, turn, plane * width)] * 2 + [near(2, held + SLOW + 1, turn, plane * width)],
            )
            around = [parts[0], parts[1], move(parts[2], middle)]
        elif kind == "R":
            (part,) = call(
                round_relay_kernel, turn * lon, turn * lon * 12,
                [vmem, vmem], [around[0], around[2]], [near(held + SLOW + 1, turn, plane * width)],
            )
            around.append(move(part, to_outer))
        elif kind == "T":
            parts = call(
                round_split_kernel, turn * lon, turn * lon * 12,
                [smem] + [vmem] * 4, [where, *around],
                [near(held + SLOW + 1, turn, width)] * plane,
            )
            around = parts[:1] + [move(parts[shift], swaps[shift]) for shift in range(1, plane)]
        elif kind == "F":
            outs = finish(functools.partial(round_final_kernel, held, matrices), turn, around, outs)
        elif kind == "p":
            first, rows = firsts[at], sizes[at]
            parts = fetch(
                [near(PLANES, held, rows, width)] * 3,
                lambda w, first=first, rows=rows: [
                    (out, 0, first, rows, step, column(w, step, shift))
                    for out, shift in ((1, 2), (2, 3), (0, 0))
                    for step in range(PLANES)
                ],
                rows,
            )
            packed[at] = [parts[0], move(parts[1], swaps[2]), move(parts[2], swaps[3])]
        elif kind == "t":
            rows = sizes[at]
            mode = next(mode for mode, chunks in GROUPS if at in chunks)
            part, offset = paired[at]
            split = any(at in chunks for chunks in NEARS)
            results = call(
                functools.partial(totals_kernel, offset, split), rows * width * PLANES * 240, rows * width * 656,
                [smem, smem] + [vmem] * plane, [where, weights, packed[at][0], part, *packed[at][1:]],
                [near(STATS, rows, width)] * (2 if split else 1) + [near(2 if split else 3, STATS, rows, width)],
            )
            home[at], own[at], far[at] = results[0], results[-2] if split else results[-1], results[-1]
            moved["a", at] = move(far[at], to_inner)
            if not split:
                moved["n", at] = (moved["a", at], 0)
            if mode == "e":
                moved["h", at] = move(home[at], to_outer)
        elif kind == "n":
            chunks = NEARS[at]
            rows = sum(sizes[chunk] for chunk in chunks)
            (part,) = call(
                functools.partial(join_kernel, len(chunks)), rows * width * 17, rows * width * 136,
                [vmem] * len(chunks), [own[chunk] for chunk in chunks], [near(STATS, rows, width)],
            )
            part = move(part, to_inner)
            for chunk in chunks:
                moved["n", chunk] = (part, sum(sizes[other] for other in chunks if other < chunk))
        elif kind == "m":
            rows = sizes[at]
            mode = next(mode for mode, chunks in GROUPS if at in chunks)
            parts = call(
                functools.partial(merge_kernel, mode == "e"), rows * width * 34, rows * width * 408,
                [vmem] * 2, [far[at], moved["a", at]],
                [near(STATS, rows, width)] * 2 if mode == "e" else [near(2, STATS, rows, width)],
            )
            moved["b", at] = move(parts[0], middle)
            if mode == "e":
                moved["g", at] = move(parts[1], across)
        elif kind == "r":
            chunks = GROUPS[at][1]
            rows = sum(sizes[chunk] for chunk in chunks)
            args = [home[chunk] for chunk in chunks] + [moved["b", chunk] for chunk in chunks]
            (part,) = call(
                functools.partial(relay_kernel, len(chunks)), rows * width * 17, rows * width * 204,
                [vmem] * len(args), args, [near(STATS, rows, width)],
            )
            moved["c", at] = move(part, to_outer)
        else:
            mode, chunks = GROUPS[at]
            rows = sum(sizes[chunk] for chunk in chunks)
            args = [home[chunk] for chunk in chunks] + [own[chunk] for chunk in chunks]
            args += [moved["n", chunk][0] for chunk in chunks] + [moved["b", chunk] for chunk in chunks]
            args += [moved["g", chunks[0]], moved["h", chunks[0]]] if mode == "e" else [moved["c", at]]
            places = [(sizes[chunk], moved["n", chunk][1]) for chunk in chunks]
            kernel = functools.partial(final_kernel, firsts[chunks[0]], places, mode, matrices)
            outs = finish(kernel, rows, args, outs)
    return tuple(outs)


def fits(groups):
    return groups == 4 * PLANES and TIMES % groups == 0 and TIMES // PLANES == 2 * PERIOD


def local(snapshots):
    groups = lax.axis_size("io")
    lat = snapshots.shape[0] * groups // TIMES
    if fits(groups) and lat % (8 * (ROUND + sum(PARTS))) == 0 and snapshots.shape[1] == 128 * groups:
        return plane_plan(snapshots)
    return general(snapshots)


def solution(mesh):
    return jax.shard_map(
        local,
        mesh=mesh,
        in_specs=(P(("rep", "io"), None),),
        out_specs=(P("rep", None, "io"), P("rep", "io")),
        check_vma=False,
    )
```

```python
import functools

import jax
import jax.numpy as jnp
import numpy as np
from jax import lax
from jax.experimental import pallas as pl
from jax.experimental.pallas import tpu as pltpu
from jax.sharding import PartitionSpec as P


TIMES = 96
HARM = 16
PERIOD = 12
SLOW = HARM - PERIOD
STATS = HARM + 1
PLANES = 4

ROUND = 4
PARTS = (4, 4, 5, 2, 4, 4, 3, 2)
GROUPS = (("s", (0, 1, 2)), ("s", (3, 4)), ("s", (5,)), ("s", (6,)), ("s", (7,)))
NEARS = ((4, 5, 6), (7,))
ORDER = " ".join((
    "P0 q0 p1 p2",
    "p3 t0 S0 p4",
    "t1 p5 m0 p6",
    "p7 t2 m1 t3",
    "R0 m2 t4 m3",
    "t5 T0 m4 r0",
    "t6 m5 t7 n0",
    "n1 m6 r1 m7",
    "F0 f0 r2 r3",
    "r4 f1 f2 f3",
    "f4",
)).split()
FINAL_ROWS = 8
VMEM_LIMIT = 8 << 20


def basis_matrix(times):
    steps = np.arange(times, dtype=np.float64)
    columns = [np.ones_like(steps), (steps - (times - 1) / 2.0) / (times / 2.0)]
    for harmonic in range(1, 7):
        columns.append(np.cos(2.0 * np.pi * harmonic * steps / 12.0))
    for harmonic in range(1, 6):
        columns.append(np.sin(2.0 * np.pi * harmonic * steps / 12.0))
    columns.append(np.cos(2.0 * np.pi * steps / times))
    columns.append(np.sin(2.0 * np.pi * steps / times))
    columns.append(np.cos(4.0 * np.pi * steps / times))
    return np.stack(columns, axis=1)


PERIODIC = [0] + list(range(2, 13))
SLOWS = [1, 13, 14, 15]


def fit_matrices():
    basis = basis_matrix(TIMES)
    to_moments = np.zeros((HARM, HARM))
    for column in PERIODIC:
        to_moments[column, :PERIOD] = basis[:PERIOD, column]
    for at, column in enumerate(SLOWS):
        to_moments[column, PERIOD + at] = 1.0
    to_coeffs = np.linalg.solve(basis.T @ basis, to_moments)
    return to_moments, to_coeffs


def fit_block(block, basis, projector):
    width = block.shape[-1]
    lat_rows = block.shape[0] // TIMES
    series = block.reshape(TIMES, lat_rows * width)
    coeffs = jnp.dot(projector, series, precision=lax.Precision.HIGHEST)
    moments = jnp.dot(basis.T, series, precision=lax.Precision.HIGHEST)
    total = jnp.sum(series * series, axis=0)
    variance = (total - jnp.sum(coeffs * moments, axis=0)) / TIMES
    return coeffs.reshape(HARM, lat_rows, width), variance.reshape(lat_rows, width)


def general(snapshots):
    groups = lax.axis_size("io")
    local_rows = snapshots.shape[0]
    lon_dev = snapshots.shape[1] // groups
    split_view = snapshots.reshape(local_rows, groups, lon_dev)
    basis = basis_matrix(TIMES)
    projector = np.linalg.solve(basis.T @ basis, basis.T)
    moved = lax.all_to_all(split_view, "io", split_axis=1, concat_axis=0, tiled=True)
    return fit_block(moved[:, 0, :], jnp.float32(basis), jnp.float32(projector))


def fetch_kernel(pieces, where_ref, x_ref, table_ref, *rest):
    count, with_table = pieces(None)
    outs, sem = rest[-2 - count : -2], rest[-1]
    copies = []
    if with_table:
        copies.append(pltpu.make_async_copy(table_ref.at[where_ref[3] * 4 + where_ref[0]], outs[-1], sem))
        copies[0].start()
    for out, to_rows, first, rows, at, column in pieces(where_ref):
        ref = outs[out] if at is None else outs[out].at[at]
        width = ref.shape[-1]
        source = x_ref.at[:, pl.ds(first, rows), pl.ds(pl.multiple_of(column, width), width)]
        copies.append(pltpu.make_async_copy(source, ref.at[:, pl.ds(to_rows, rows)], sem))
        copies[-1].start()
    for copy in copies:
        copy.wait()


def sums(values, weights, way, emit):
    slow, square = [None] * SLOW, None
    held = len(values[0])
    for k in range(held):
        for at, source in enumerate(values):
            for j in range(SLOW):
                term = source[k] * weights[way * SLOW + j, at * held + k]
                slow[j] = term if slow[j] is None else slow[j] + term
            term = source[k] * source[k]
            square = term if square is None else square + term
    for j in range(SLOW):
        emit(j, slow[j])
    emit(SLOW, square)


def row_blocks(rows, body):
    size = 16 if rows % 16 == 0 else 8

    @pl.loop(0, rows // size)
    def _(block):
        body(block * size, size)


def totals_kernel(offset, split, where_ref, weight_ref, own_ref, r1_ref, r2_ref, r3_ref, *rest):
    home_ref, near_ref, far_ref = rest[-4:-1] if split else (rest[-3], None, rest[-2])
    held, rows = own_ref.shape[1:3]
    first = (where_ref[0] % 2) * held
    second = held - first
    for step in range(PLANES):
        out_ref = (home_ref, near_ref if near_ref is not None else far_ref.at[2], far_ref.at[0], far_ref.at[1])[step]

        def body(start, size):
            at, at1 = pl.ds(pl.multiple_of(start, 8), size), pl.ds(pl.multiple_of(start + offset, 8), size)
            values = [
                [ref[step, k, rows_] for k in range(held)]
                for ref, rows_ in ((own_ref, at), (r1_ref, at1), (r2_ref, at), (r3_ref, at))
            ]
            for k in range(held):
                out_ref[first + k, at] = values[0][k] + values[2][k]
                out_ref[second + k, at] = values[1][k] + values[3][k]

            def emit(row, value):
                out_ref[PERIOD + row, at] = value

            sums(values, weight_ref, 0, emit)

        row_blocks(rows, body)


def round_sums_kernel(where_ref, weight_ref, own_ref, in_ref, *rest):
    home_ref, near_ref, far_ref = rest[-4:-1]
    held, rows = own_ref.shape[1:3]
    width = 128
    for step in range(PLANES):
        out_ref = (home_ref, near_ref, far_ref.at[0], far_ref.at[1])[step]
        for part in range(own_ref.shape[3] // width):
            columns = slice(part * width, (part + 1) * width)

            def body(start, size):
                at = pl.ds(pl.multiple_of(start, 8), size)
                values = [[own_ref[step, k, at, columns] for k in range(held)]]
                if step > 0:
                    values.append([in_ref[step - 1, k, at, columns] for k in range(held)])
                for k in range(held):
                    out_ref[k, at, columns] = values[0][k] + values[1][k] if step > 0 else values[0][k]

                def emit(row, value):
                    out_ref[held + row, at, columns] = value

                sums(values, weight_ref, 1, emit)

            row_blocks(rows, body)


def round_relay_kernel(home_ref, b_ref, *rest):
    rest[-2][...] = home_ref[...] + b_ref[1]


def round_split_kernel(where_ref, home_ref, near_ref, b_ref, c_ref, *rest):
    outs = rest[-5:-1]
    width = outs[0].shape[-1]
    for shift, out_ref in enumerate(outs):
        column = pl.ds(pl.multiple_of((where_ref[0] ^ shift) * width, width), width)

        @pl.when(where_ref[1] > 0)
        def _():
            out_ref[...] = near_ref[:, :, column] + b_ref[0, :, :, column]

        @pl.when(where_ref[1] == 0)
        def _():
            out_ref[...] = home_ref[:, :, column] + c_ref[:, :, column]


def join_kernel(count, *refs):
    out_ref, start = refs[-2], 0
    for ref in refs[:count]:
        rows = ref.shape[1]
        out_ref[:, start : start + rows] = ref[...]
        start += rows


def merge_kernel(straight, own_ref, in_ref, *rest):
    outs = rest[-3:-1] if straight else rest[-2:-1]
    for hop in range(2):
        out_ref = outs[hop] if straight else outs[0].at[hop]
        out_ref[...] = own_ref[hop] + in_ref[hop]


def relay_kernel(count, *refs):
    out_ref, start = refs[-2], 0
    for home_ref, b_ref in zip(refs[:count], refs[count : 2 * count]):
        rows = home_ref.shape[1]
        out_ref[:, start : start + rows] = home_ref[...] + b_ref[1]
        start += rows


def solve(matrices, coeff_ref, var_ref, start, rows, load):
    to_moments, to_coeffs = matrices

    @pl.loop(0, rows // FINAL_ROWS)
    def _(block):
        at = pl.multiple_of(block * FINAL_ROWS, FINAL_ROWS)
        stats = [load(row, at) for row in range(STATS)]

        def mix(weights):
            total = None
            for weight, stat in zip(weights, stats):
                if abs(weight) > 1e-12:
                    term = stat if weight == 1.0 else stat * np.float32(weight)
                    total = term if total is None else total + term
            return total

        to = pl.ds(pl.multiple_of(start + at, FINAL_ROWS), FINAL_ROWS)
        explained = None
        for column in range(HARM):
            coeff = mix(to_coeffs[column])
            coeff_ref[column, to] = coeff
            term = coeff * mix(to_moments[column])
            explained = term if explained is None else explained + term
        var_ref[to] = (stats[HARM] - explained) * np.float32(1.0 / TIMES)


def store(first, coeff_out, var_out, coeff_ref, var_ref, sem):
    rows = var_ref.shape[0]
    copies = [
        pltpu.make_async_copy(coeff_ref, coeff_out.at[:, pl.ds(first, rows)], sem.at[0]),
        pltpu.make_async_copy(var_ref, var_out.at[pl.ds(first, rows)], sem.at[1]),
    ]
    for copy in copies:
        copy.start()
    for copy in copies:
        copy.wait()


def final_kernel(first, chunks, mode, matrices, where_ref, *refs):
    coeff_out, var_out, _, coeff_ref, var_ref, sem = refs[-6:]
    count = len(chunks)
    homes, owns, nears = refs[:count], refs[count : 2 * count], refs[2 * count : 3 * count]
    middles, two_ref = refs[3 * count : 4 * count], refs[4 * count]

    @pl.when(where_ref[1] > 0)
    def _():
        start = 0
        for (rows, place), own_ref, in_ref, b_ref in zip(chunks, owns, nears, middles):

            def load(row, at, place=place, own_ref=own_ref, in_ref=in_ref, b_ref=b_ref):
                middle = b_ref if mode == "e" else b_ref.at[0]
                own_part, in_part = (ref if len(ref.shape) == 3 else ref.at[2] for ref in (own_ref, in_ref))
                value = own_part[row, pl.ds(at, FINAL_ROWS)] + in_part[row, pl.ds(pl.multiple_of(at + place, 8), FINAL_ROWS)]
                return value + middle[row, pl.ds(at, FINAL_ROWS)]

            solve(matrices, coeff_ref, var_ref, start, rows, load)
            start += rows

    @pl.when(where_ref[1] == 0)
    def _():
        start = 0
        for (rows, place), home_ref in zip(chunks, homes):

            def load(row, at, start=start, home_ref=home_ref):
                value = home_ref[row, pl.ds(at, FINAL_ROWS)] + two_ref[row, pl.ds(pl.multiple_of(at + start, 8), FINAL_ROWS)]
                if mode == "e":
                    value = value + refs[4 * count + 1][row, pl.ds(at, FINAL_ROWS)]
                return value

            solve(matrices, coeff_ref, var_ref, start, rows, load)
            start += rows

    store(first, coeff_out, var_out, coeff_ref, var_ref, sem)


def round_final_kernel(held, matrices, where_ref, *refs):
    coeff_out, var_out, _, coeff_ref, var_ref, sem = refs[-6:]
    rows = var_ref.shape[0]

    def run(early, late):
        def load(row, at):
            rows_ = pl.ds(at, FINAL_ROWS)
            if row < PERIOD:
                one, two = early if row < held else late
                return one[row % held, rows_] + two[row % held, rows_]
            row = row - PERIOD + held
            return (refs[0][row, rows_] + refs[1][row, rows_]) + (refs[2][row, rows_] + refs[3][row, rows_])

        solve(matrices, coeff_ref, var_ref, 0, rows, load)

    @pl.when(where_ref[0] % 2 == 0)
    def _():
        run((refs[0], refs[2]), (refs[1], refs[3]))

    @pl.when(where_ref[0] % 2 == 1)
    def _():
        run((refs[1], refs[3]), (refs[0], refs[2]))

    store(0, coeff_out, var_out, coeff_ref, var_ref, sem)


def plane_plan(snapshots):
    groups = lax.axis_size("io")
    plane = groups // PLANES
    held = TIMES // groups
    lat = snapshots.shape[0] // held
    lon = snapshots.shape[1]
    width = lon // groups
    view = snapshots.reshape(held, lat, lon)

    me = lax.axis_index("io")
    place, level = me % plane, me // plane
    flip = (level >= PLANES // 2).astype(jnp.int32)
    inner = ((level > 0) & (level < PLANES - 1)).astype(jnp.int32)
    where = jnp.stack([place, inner, flip, level]).astype(jnp.int32)

    slow = basis_matrix(TIMES)[:, SLOWS].T
    table = np.zeros((groups, 2 * SLOW, plane * held), np.float32)
    for device in range(groups):
        for shift in range(plane):
            for way, other in enumerate((device ^ shift, device ^ (shift * plane))):
                rows, columns = way * SLOW, shift * held
                table[device, rows : rows + SLOW, columns : columns + held] = slow[:, other * held : (other + 1) * held]
    table = jnp.asarray(table)
    matrices = fit_matrices()

    smem = pl.BlockSpec(memory_space=pltpu.SMEM)
    vmem = pl.BlockSpec(memory_space=pltpu.VMEM)
    hbm = pl.BlockSpec(memory_space=pltpu.HBM)
    space = {id(vmem): pltpu.VMEM, id(hbm): pltpu.HBM}
    token = []

    def near(*dims):
        return pltpu.VMEM(dims, jnp.float32)

    def call(kernel, flops, moved, ins, args, outs, out_specs=None, **more):
        ins, args = ins + [hbm] * len(token), list(args) + token
        args = [
            pltpu.with_memory_space_constraint(arg, space[id(spec)]) if id(spec) in space else arg
            for spec, arg in zip(ins, args)
        ]
        *results, last = pl.pallas_call(
            kernel,
            in_specs=ins,
            out_specs=(out_specs or [vmem] * len(outs)) + [hbm],
            out_shape=outs + [pltpu.HBM((8, 128), jnp.float32)],
            cost_estimate=pl.CostEstimate(flops=flops, bytes_accessed=moved, transcendentals=0),
            compiler_params=pltpu.CompilerParams(vmem_limit_bytes=VMEM_LIMIT),
            **more,
        )(*args)
        token[:] = [last]
        return results

    def move(value, pairs):
        return lax.ppermute(value, "io", pairs)

    unit = lat // (ROUND + sum(PARTS))
    sizes = [part * unit for part in PARTS]
    firsts = [(ROUND + sum(PARTS[:chunk])) * unit for chunk in range(len(PARTS))]
    turn = ROUND * unit
    swaps = [[(i, i ^ shift) for i in range(groups)] for shift in range(plane)]
    to_inner = [(i, i + plane) for i in range(plane)] + [(i, i - plane) for i in range(groups - plane, groups)]
    to_outer = [(b, a) for a, b in to_inner]
    middle = [(i, i + plane) for i in range(plane, 2 * plane)]
    middle = middle + [(b, a) for a, b in middle]
    across = [(i, i + 2 * plane) for i in range(plane, 2 * plane)]
    across = across + [(i, i - 2 * plane) for i in range(2 * plane, 3 * plane)]

    def fetch(outs, pieces, rows, with_table=False):
        outs = outs + [near(2 * SLOW, plane * held)] * with_table

        def count_or_pieces(where_ref):
            return (len(outs), with_table) if where_ref is None else pieces(where_ref)

        return call(
            functools.partial(fetch_kernel, count_or_pieces), rows * lon, rows * lon * held * 8,
            [smem, hbm, hbm], [where, view, table], outs, scratch_shapes=[pltpu.SemaphoreType.DMA],
        )

    def pieces_of(w, out, first, rows, shift):
        return [(out, 0, first, rows, step, column(w, step, shift)) for step in range(PLANES)]

    def column(where_ref, step, shift):
        zone = jnp.where(where_ref[2] > 0, PLANES - 1 - step, step)
        return (zone * plane + (where_ref[0] ^ shift)) * width

    def finish(kernel, rows, args, outs):
        count = len(args)
        return call(
            kernel, rows * width * 832, rows * width * 272,
            [smem] + [vmem] * count + [hbm] * len(outs), [where, *args, *outs],
            [pltpu.HBM((HARM, lat, width), jnp.float32), pltpu.HBM((lat, width), jnp.float32)], [hbm, hbm],
            input_output_aliases={count + 1: 0, count + 2: 1} if outs else {},
            scratch_shapes=[
                pltpu.VMEM((HARM, rows, width), jnp.float32),
                pltpu.VMEM((rows, width), jnp.float32),
                pltpu.SemaphoreType.DMA((2,)),
            ],
        )

    packed, home, own, far, moved, outs = {}, {}, {}, {}, {}, []
    for item in ORDER:
        kind, at = item[0], int(item[1:])
        if kind == "P":
            first, rows = firsts[0], sizes[0]
            parts = fetch(
                [near(PLANES - 1, held, turn, plane * width)] + [near(PLANES, held, rows, width)] * 2,
                lambda w: [(0, 0, 0, turn, step - 1, column(w, step, w[0])) for step in (1, 2, 3)]
                + pieces_of(w, 1, first, rows, 2) + pieces_of(w, 2, first, rows, 3),
                turn + rows,
            )
            around = [None, move(parts[0], to_inner)]
            packed[0] = [None, move(parts[1], swaps[2]), move(parts[2], swaps[3])]
        elif kind == "q":
            first, rows, own_rows = firsts[0], sum(sizes), sizes[0]
            parts = fetch(
                [near(PLANES, held, rows, width), near(PLANES, held, turn, plane * width), near(PLANES, held, own_rows, width)],
                lambda w: pieces_of(w, 0, first, rows, 1)
                + [(1, 0, 0, turn, step, column(w, step, w[0])) for step in range(PLANES)]
                + pieces_of(w, 2, first, own_rows, 0),
                rows, True,
            )
            part = move(parts[0], swaps[1])
            around[0], packed[0][0], weights = parts[1], parts[2], parts[3]
            paired = [(part, other - first) for other in firsts]
        elif kind == "S":
            parts = call(
                round_sums_kernel, turn * lon * 40, turn * lon * held * 8,
                [smem, smem, vmem, vmem], [where, weights, *around],
                [near(held + SLOW + 1, turn, plane * width)] * 2 + [near(2, held + SLOW + 1, turn, plane * width)],
            )
            around = [parts[0], parts[1], move(parts[2], middle)]
        elif kind == "R":
            (part,) = call(
                round_relay_kernel, turn * lon, turn * lon * 12,
                [vmem, vmem], [around[0], around[2]], [near(held + SLOW + 1, turn, plane * width)],
            )
            around.append(move(part, to_outer))
        elif kind == "T":
            parts = call(
                round_split_kernel, turn * lon, turn * lon * 12,
                [smem] + [vmem] * 4, [where, *around],
                [near(held + SLOW + 1, turn, width)] * plane,
            )
            around = parts[:1] + [move(parts[shift], swaps[shift]) for shift in range(1, plane)]
        elif kind == "F":
            outs = finish(functools.partial(round_final_kernel, held, matrices), turn, around, outs)
        elif kind == "p":
            first, rows = firsts[at], sizes[at]
            parts = fetch(
                [near(PLANES, held, rows, width)] * 3,
                lambda w, first=first, rows=rows: [
                    (out, 0, first, rows, step, column(w, step, shift))
                    for out, shift in ((1, 2), (2, 3), (0, 0))
                    for step in range(PLANES)
                ],
                rows,
            )
            packed[at] = [parts[0], move(parts[1], swaps[2]), move(parts[2], swaps[3])]
        elif kind == "t":
            rows = sizes[at]
            mode = next(mode for mode, chunks in GROUPS if at in chunks)
            part, offset = paired[at]
            split = any(at in chunks for chunks in NEARS)
            results = call(
                functools.partial(totals_kernel, offset, split), rows * width * PLANES * 240, rows * width * 656,
                [smem, smem] + [vmem] * plane, [where, weights, packed[at][0], part, *packed[at][1:]],
                [near(STATS, rows, width)] * (2 if split else 1) + [near(2 if split else 3, STATS, rows, width)],
            )
            home[at], own[at], far[at] = results[0], results[-2] if split else results[-1], results[-1]
            moved["a", at] = move(far[at], to_inner)
            if not split:
                moved["n", at] = (moved["a", at], 0)
            if mode == "e":
                moved["h", at] = move(home[at], to_outer)
        elif kind == "n":
            chunks = NEARS[at]
            rows = sum(sizes[chunk] for chunk in chunks)
            (part,) = call(
                functools.partial(join_kernel, len(chunks)), rows * width * 17, rows * width * 136,
                [vmem] * len(chunks), [own[chunk] for chunk in chunks], [near(STATS, rows, width)],
            )
            part = move(part, to_inner)
            for chunk in chunks:
                moved["n", chunk] = (part, sum(sizes[other] for other in chunks if other < chunk))
        elif kind == "m":
            rows = sizes[at]
            mode = next(mode for mode, chunks in GROUPS if at in chunks)
            parts = call(
                functools.partial(merge_kernel, mode == "e"), rows * width * 34, rows * width * 408,
                [vmem] * 2, [far[at], moved["a", at]],
                [near(STATS, rows, width)] * 2 if mode == "e" else [near(2, STATS, rows, width)],
            )
            moved["b", at] = move(parts[0], middle)
            if mode == "e":
                moved["g", at] = move(parts[1], across)
        elif kind == "r":
            chunks = GROUPS[at][1]
            rows = sum(sizes[chunk] for chunk in chunks)
            args = [home[chunk] for chunk in chunks] + [moved["b", chunk] for chunk in chunks]
            (part,) = call(
                functools.partial(relay_kernel, len(chunks)), rows * width * 17, rows * width * 204,
                [vmem] * len(args), args, [near(STATS, rows, width)],
            )
            moved["c", at] = move(part, to_outer)
        else:
            mode, chunks = GROUPS[at]
            rows = sum(sizes[chunk] for chunk in chunks)
            args = [home[chunk] for chunk in chunks] + [own[chunk] for chunk in chunks]
            args += [moved["n", chunk][0] for chunk in chunks] + [moved["b", chunk] for chunk in chunks]
            args += [moved["g", chunks[0]], moved["h", chunks[0]]] if mode == "e" else [moved["c", at]]
            places = [(sizes[chunk], moved["n", chunk][1]) for chunk in chunks]
            kernel = functools.partial(final_kernel, firsts[chunks[0]], places, mode, matrices)
            outs = finish(kernel, rows, args, outs)
    return tuple(outs)


def fits(groups):
    return groups == 4 * PLANES and TIMES % groups == 0 and TIMES // PLANES == 2 * PERIOD


def local(snapshots):
    groups = lax.axis_size("io")
    lat = snapshots.shape[0] * groups // TIMES
    if fits(groups) and lat % (8 * (ROUND + sum(PARTS))) == 0 and snapshots.shape[1] == 128 * groups:
        return plane_plan(snapshots)
    return general(snapshots)


def solution(mesh):
    return jax.shard_map(
        local,
        mesh=mesh,
        in_specs=(P(("rep", "io"), None),),
        out_specs=(P("rep", None, "io"), P("rep", "io")),
        check_vma=False,
    )
```
